256 devices in a mesh: grp: 2 (over z), seq: 16 (over y, core), head: 8 (over x).
Axes of the slice: x: 8, y: 8, z: 2, core: 2. Of those that a mesh axis runs over, the one named last changes fastest.
The devices are a block of a 8x8x16 slice.
Arguments:
- q_latent: bfloat16 [32, 128, 512], P(('grp', 'seq'), 'head'), parts along dimension 0, may hold values from -6 to 6
- q_rope: bfloat16 [32, 128, 64], P(('grp', 'seq'), 'head'), parts along dimension 0, may hold values from -6 to 6
- cache_latent: bfloat16 [9216, 128, 512], P(('grp', 'seq', 'head')), parts along dimension 0, may hold values from -6 to 6
- cache_rope: bfloat16 [9216, 64, 128], P(('grp', 'seq', 'head')), parts along dimension 0, may hold values from -6 to 6
- page_table: int32 [32, 512], P(('grp', 'seq')), parts along dimension 0, may hold values from -1 to 4607, as said below
- lengths: int32 [32], P(('grp', 'seq')), parts along dimension 0, may hold values from 1 to 65536, as said below
Outputs:
- attended: bfloat16 [32, 128, 512], P(('grp', 'seq'), 'head'), parts along dimension 0
The draws below stay inside these ranges and needn't reach their ends.
There are 2 independent parts, one for each index of `grp`. The reference program is written for one: setup_inputs(seed, part) draws one part's arguments, and reference() takes and returns one part's arrays. A program takes and returns all parts, laid end to end along the dimension named above; each array names one. Nothing has to cross between parts.
Inputs may be any that keep to these rules, and one draw needn't show every extreme that they name: `page_table`: row s holds the pool slots of the pages of sequence s in page order; entries from ceil(lengths[s] / 128) on are -1; no slot appears twice in the table. Slots d * 36 to (d + 1) * 36 - 1 belong to device d of seq+head (seq index first). One device holds at most 4 pages of one sequence; one sequence has exactly 4 pages on every device. Sequence s has ceil(lengths[s] / 128) pages; the sequence with 4 pages on every device has length 65536.
All inputs are finite; a program needn't handle non-finite values.
Results may differ from the reference program's by a relative error of at most 0.007.
Values may be sent and summed in bfloat16 or wider, within the bound.
A program may use at most 64 MiB of HBM per device.

```python
import jax
import jax.numpy as jnp
from jax import lax

HEADS = 128
LAT = 512
ROPE = 64
PAGE = 128
SLOTS = 36
SEQS = 16
NODES = 128
SLOTS_ALL = 4608
SHARE = 2
MOST = 4
MAXP = 512


def pool_layout(key):
    key_list = jax.random.split(jax.random.fold_in(key, 23), 8)
    device_level = jax.random.randint(key_list[0], (NODES, 1), 1, 5)
    base_count = jax.random.randint(key_list[1], (NODES, SEQS), 0, SHARE + 1)
    page_counts = base_count * device_level // 4
    hot_seq = jax.random.randint(key_list[2], (), 0, SEQS)
    fuller = jax.random.randint(key_list[3], (), 0, NODES)
    seq_column = jnp.arange(SEQS, dtype=jnp.int32)[None, :]
    node_ids = jnp.arange(NODES, dtype=jnp.int32)[:, None]
    page_counts = jnp.where(node_ids == fuller, SHARE, page_counts)
    page_counts = jnp.where(seq_column == hot_seq, MOST, page_counts)
    within = jnp.arange(MOST, dtype=jnp.int32)
    used = within[None, None, :] < page_counts[:, :, None]
    flat_width = SEQS * MOST
    noise_one = jax.random.randint(key_list[4], (NODES, flat_width), 0, 2 ** 30 // flat_width)
    entry_ids = jnp.arange(flat_width, dtype=jnp.int32)[None, :]
    rank_keys = jnp.where(used.reshape(NODES, flat_width), noise_one * flat_width + entry_ids, 2 ** 30 + entry_ids)
    ranking = jnp.argsort(jnp.argsort(rank_keys, axis=1), axis=1)
    slot_noise = jax.random.randint(key_list[5], (NODES, SLOTS), 0, 2 ** 30 // SLOTS)
    slot_perm = jnp.argsort(slot_noise * SLOTS + jnp.arange(SLOTS, dtype=jnp.int32)[None, :], axis=1)
    local_slot = jnp.take_along_axis(slot_perm, jnp.minimum(ranking, SLOTS - 1), axis=1)
    global_slot = (node_ids * SLOTS + local_slot).reshape(NODES, SEQS, MOST)
    cand_slot = jnp.transpose(global_slot, (1, 0, 2)).reshape(SEQS, MAXP)
    cand_used = jnp.transpose(used, (1, 0, 2)).reshape(SEQS, MAXP)
    noise_two = jax.random.randint(key_list[6], (SEQS, MAXP), 0, 2 ** 30 // MAXP)
    spots = jnp.arange(MAXP, dtype=jnp.int32)[None, :]
    order_keys = jnp.where(cand_used, noise_two * MAXP + spots, 2 ** 30 + spots)
    picked = jnp.argsort(order_keys, axis=1)
    table = jnp.take_along_axis(cand_slot, picked, axis=1)
    page_total = jnp.sum(page_counts, axis=0)
    table = jnp.where(spots < page_total[:, None], table, -1)
    last_fill = jax.random.randint(key_list[7], (SEQS,), 1, PAGE + 1)
    last_fill = jnp.where(jnp.arange(SEQS, dtype=jnp.int32) == hot_seq, PAGE, last_fill)
    seq_lengths = (page_total - 1) * PAGE + last_fill
    return (table.astype(jnp.int32), seq_lengths.astype(jnp.int32))


def draw_page_table(key, part):
    return pool_layout(key)[0]


def draw_lengths(key, part):
    return pool_layout(key)[1]


def draw_q_latent(key, part):
    own_key = jax.random.fold_in(key, 31)
    values = jax.random.truncated_normal(own_key, -6.0, 6.0, (SEQS, HEADS, LAT), jnp.float32)
    return values.astype(jnp.bfloat16)


def draw_cache_latent(key, part):
    noise = jax.random.truncated_normal(jax.random.fold_in(key, 41), -6.0, 6.0, (SLOTS_ALL, PAGE, LAT), jnp.float32)
    values = noise
    return values.astype(jnp.bfloat16)


def block_levels(rng, extent, cuts, least, top_value):
    loudness, own = 1.0, jax.random.fold_in(rng, 6)
    for dim, parts in cuts:
        heights = jnp.exp(jax.random.uniform(jax.random.fold_in(own, dim), (parts,), jnp.float32, least / len(cuts), top_value / len(cuts)))
        loudness = loudness * jnp.repeat(heights, extent[dim] // parts).reshape([-1 if axis == dim else 1 for axis in range(len(extent))])
    return loudness


def centred(key, extent, spread, most, shards=(), kind=jnp.bfloat16):
    result = spread * jax.random.normal(key, extent, jnp.float32)
    if shards:
        result = result * block_levels(key, extent, shards, -0.22, 0.18)
    return jnp.clip(result, -most, most).astype(kind)


def setup_inputs(seed: int = 0, part: int = 0) -> dict:
    key_of = jax.random.split(jax.random.key(seed), 7)
    own_keys = jax.random.split(jax.random.fold_in(key_of[6], part), 7)
    return {
        "q_latent": draw_q_latent(jax.random.fold_in(jax.random.fold_in(key_of[6], part), 71), part),
        "q_rope": centred(own_keys[1], (SEQS, HEADS, ROPE), 1.0, 6.0, ((0, 16), (1, 8))),
        "cache_latent": draw_cache_latent(jax.random.fold_in(jax.random.fold_in(key_of[6], part), 71), part),
        "cache_rope": centred(own_keys[3], (SLOTS_ALL, ROPE, PAGE), 1.0, 6.0, ((0, 128),)),
        "page_table": draw_page_table(jax.random.fold_in(jax.random.fold_in(key_of[6], part), 71), part),
        "lengths": draw_lengths(jax.random.fold_in(jax.random.fold_in(key_of[6], part), 71), part),
    }


softmax_scale = 0.13528
floor_score = -1.0e30
page_block = 32


def one_sequence(query_lat, query_rot, table_row, length, cache_latent, cache_rope):
    page_len = cache_latent.shape[1]
    lat_width = cache_latent.shape[2]
    row_width = table_row.shape[0]
    padded_width = ((row_width + page_block - 1) // page_block) * page_block
    table_row = jnp.concatenate([table_row.astype(jnp.int32), jnp.full((padded_width - row_width,), -1, jnp.int32)])
    block_rows = table_row.reshape(padded_width // page_block, page_block)
    first_pages = jnp.arange(padded_width // page_block, dtype=jnp.int32) * page_block
    query_lat = query_lat.astype(jnp.float32)
    query_rot = query_rot.astype(jnp.float32)
    head_count = query_lat.shape[0]
    token_offset = jnp.arange(page_len, dtype=jnp.int32)
    block_pages = jnp.arange(page_block, dtype=jnp.int32)

    def block_scores(inputs):
        start_page, slot_ids = inputs

        def compute(operand):
            safe_ids = jnp.maximum(slot_ids, 0)
            latent = cache_latent[safe_ids].astype(jnp.float32)
            rotary = cache_rope[safe_ids].astype(jnp.float32)
            scores = jnp.einsum("hd,btd->hbt", query_lat, latent, precision=lax.Precision.HIGHEST)
            scores = scores + jnp.einsum("he,bet->hbt", query_rot, rotary, precision=lax.Precision.HIGHEST)
            position = (start_page + block_pages)[:, None] * page_len + token_offset[None, :]
            usable = (slot_ids[:, None] >= 0) & (position < length)
            return jnp.where(usable[None], scores * softmax_scale, floor_score).reshape(head_count, page_block * page_len)

        def skipped(operand):
            return jnp.full((head_count, page_block * page_len), floor_score, jnp.float32)

        return lax.cond(start_page * page_len < length, compute, skipped, 0)

    all_scores = lax.map(block_scores, (first_pages, block_rows))
    best_top = jnp.max(all_scores, axis=(0, 2))

    def block_mix(carry, inputs):
        start_page, slot_ids, scores = inputs

        def compute(operand):
            latent = cache_latent[jnp.maximum(slot_ids, 0)].reshape(page_block * page_len, lat_width)
            weight = jnp.exp(scores - best_top[:, None])
            total_part = jnp.sum(weight, axis=1)
            mixed_part = jnp.dot(weight.astype(jnp.bfloat16), latent, preferred_element_type=jnp.float32)
            return total_part, mixed_part

        def skipped(operand):
            return jnp.zeros((head_count,), jnp.float32), jnp.zeros((head_count, lat_width), jnp.float32)

        total_part, mixed_part = lax.cond(start_page * page_len < length, compute, skipped, 0)
        return (carry[0] + total_part, carry[1] + mixed_part), None

    start_carry = (jnp.zeros((head_count,), jnp.float32), jnp.zeros((head_count, lat_width), jnp.float32))
    (total_sum, mixed_sum), unused = lax.scan(block_mix, start_carry, (first_pages, block_rows, all_scores))
    return (mixed_sum / total_sum[:, None]).astype(jnp.bfloat16)


def reference(q_latent, q_rope, cache_latent, cache_rope, page_table, lengths):
    def per_sequence(inputs):
        query_lat, query_rot, table_row, length = inputs
        return one_sequence(query_lat, query_rot, table_row, length, cache_latent, cache_rope)

    return lax.map(per_sequence, (q_latent, q_rope, page_table, lengths))
```

```python
import functools

import jax
import jax.numpy as jnp
from jax import lax
from jax.experimental import pallas as pl
from jax.experimental.pallas import tpu as pltpu
from jax.sharding import PartitionSpec as P

softmax_scale = 0.13528
floor_score = -1e30
MESH = pl.DeviceIdType.MESH
MOST = 4
STAT = 128
bf16, f32 = jnp.bfloat16, jnp.float32


def kernel(
    n, heads, lat_w, rope_w, page, slots,
    q_hbm, t_hbm, lat_hbm, rope_hbm,
    out_ref,
    lat, rope, QB, TB, PB, RB, RR, MS, M2, FB, tvm, tsm,
    loc, a_send, a_recv, t_send, t_recv, g_send, g_recv, d_send, d_recv, td_send, td_recv,
    p_send, p_recv, r_send, r_recv, f_send, f_recv,
):
    half = n // 2
    sq = lax.axis_index("seq")
    x = lax.axis_index("head")
    y = sq // 2
    c = sq % 2
    a = x * (1 - c) + y * c
    b = y * (1 - c) + x * c

    def at(xx, yy, cc):
        return {"seq": 2 * yy + cc, "head": xx}

    def dev_a(i):
        return at(i * (1 - c) + x * c, y * (1 - c) + i * c, c)

    def dev_b(i):
        return at(x * (1 - c) + i * c, i * (1 - c) + y * c, c)

    sib = at(x, y, 1 - c)

    def rcopy(src, dst, ss, rs, dev):
        return pltpu.make_async_remote_copy(
            src_ref=src, dst_ref=dst, send_sem=ss, recv_sem=rs, device_id=dev, device_id_type=MESH
        )

    sends = []

    def send(src, dst, ss, rs, dev):
        cp = rcopy(src, dst, ss, rs, dev)
        cp.start()
        sends.append(cp)

    cq = pltpu.make_async_copy(q_hbm, QB.at[c, b, a], loc.at[0])
    ct = pltpu.make_async_copy(t_hbm, TB.at[c, y], loc.at[1])
    cl = pltpu.make_async_copy(lat_hbm, lat, loc.at[2])
    cr = pltpu.make_async_copy(rope_hbm, rope, loc.at[3])
    cq.start()
    ct.start()
    cl.start()
    cr.start()

    bar = pltpu.get_barrier_semaphore()
    for k in range(1, n):
        pl.semaphore_signal(bar, inc=1, device_id=dev_a((a + k) % n), device_id_type=MESH)
        pl.semaphore_signal(bar, inc=1, device_id=dev_b((b + k) % n), device_id_type=MESH)
    pl.semaphore_signal(bar, inc=1, device_id=sib, device_id_type=MESH)
    pl.semaphore_wait(bar, 2 * (n - 1) + 1)

    far = sorted(range(1, n), key=lambda k: -min(k, n - k))
    cq.wait()
    for k in far:
        send(QB.at[c, b, a], QB.at[c, b, a], a_send.at[k], a_recv.at[k], dev_a((a + k) % n))
    ct.wait()
    for k in far:
        send(TB.at[c, y], TB.at[c, y], t_send.at[k], t_recv.at[k], at(x, (y + k) % n, c))
    for k in far:
        rcopy(
            QB.at[c, b, (a - k) % n], QB.at[c, b, (a - k) % n], a_send.at[k], a_recv.at[k], sib
        ).wait_recv()

    def gpart(idx, h):
        return QB.at[c, idx, pl.ds(h * half, half)]

    right, left = dev_b((b + 1) % n), dev_b((b + n - 1) % n)
    nxt = (right, left)

    def origin(d, k):
        return (b + n - k) % n if d == 0 else (b + k) % n

    for h in range(2):
        for d in range(2):
            send(gpart(b, h), gpart(b, h), g_send.at[d, h], g_recv.at[d, h], nxt[d])
    send(QB.at[c, b], QB.at[c, b], d_send.at[2 * (n - 1)], d_recv.at[2 * (n - 1)], sib)

    for k in far:
        rcopy(
            TB.at[c, (y - k) % n], TB.at[c, (y - k) % n], t_send.at[k], t_recv.at[k], sib
        ).wait_recv()
    send(TB.at[c], TB.at[c], td_send.at[0], td_recv.at[0], sib)

    def ring_step(k):
        for j in range(2):
            for d in range(2):
                if k == half:
                    if j == 1:
                        continue
                    h, i = d, 2 * (half - 1)
                else:
                    h = j if d == 0 else 1 - j
                    i = 2 * (k - 1) + h
                part = gpart(origin(d, k), h)
                rcopy(part, part, g_send.at[d, i], g_recv.at[d, i], sib).wait_recv()
                if k < half - 1:
                    send(part, part, g_send.at[d, i + 2], g_recv.at[d, i + 2], nxt[d])
                elif k == half - 1 and h == d:
                    i2 = 2 * (half - 1)
                    send(part, part, g_send.at[d, i2], g_recv.at[d, i2], nxt[d])
                dd = d * (n - 1) + i
                send(part, part, d_send.at[dd], d_recv.at[dd], sib)

    b_sib = y * c + x * (1 - c)

    def d2d_wait(k):
        if k == 0:
            part = QB.at[1 - c, b_sib]
            i = 2 * (n - 1)
            rcopy(part, part, d_send.at[i], d_recv.at[i], sib).wait_recv()
            return
        for d in range(2):
            o = (b_sib + n - k) % n if d == 0 else (b_sib + k) % n
            for h in range(2):
                if k == half and h != d:
                    continue
                i = 2 * (k - 1) + h if k < half else 2 * (half - 1)
                part = QB.at[1 - c, o, pl.ds(h * half, half)]
                rcopy(
                    part, part, d_send.at[d * (n - 1) + i], d_recv.at[d * (n - 1) + i], sib
                ).wait_recv()

    def build_table():
        first = (sq * n + x) * slots * 256
        codes = TB[...].reshape(n * 16, 128)
        ok = (codes >= first) & (codes < first + slots * 256)
        key = jnp.where(ok, codes - first, -1).T
        row = lax.broadcasted_iota(jnp.int32, (8, 128), 0)
        lane = lax.broadcasted_iota(jnp.int32, (8, 128), 1)
        res = jnp.full((8, 128), -1, jnp.int32)
        for j in range(MOST):
            m = key
            size = key.shape[0]
            while size > 8:
                size //= 2
                m = jnp.maximum(m[:size], m[size:])
            for r in (4, 2, 1):
                m = jnp.maximum(m, pltpu.roll(m, r, 0))
            for bit in (1, 2, 4):
                part = jnp.where((lane & bit) > 0, pltpu.roll(m, bit, 1), pltpu.roll(m, 128 - bit, 1))
                m = jnp.maximum(m, part)
            res = jnp.where(row == j, m, res)
            key = jnp.where(key == jnp.concatenate([m] * 16, axis=0), -1, key)
        tvm[...] = res
        cp = pltpu.make_async_copy(tvm, tsm, loc.at[4])
        cp.start()
        cp.wait()

    def compute(par, yy):
        q = (QB[0, yy] if par == 0 else QB[1, :, yy]).reshape(n * heads, -1)
        ql, qr = q[:, :lat_w], q[:, lat_w : lat_w + rope_w]
        pages, parts = [], []
        lane = lax.broadcasted_iota(jnp.int32, (n * heads, page), 1)
        live = []
        for j in range(MOST):
            code = tsm[j, 8 * (par * n + yy)]
            slot = jnp.maximum(code, 0) // 256
            count = jnp.where(code < 0, 0, code % 256)
            pg = lat[slot]
            pages.append(pg)
            sc = lax.dot_general(ql, pg, (((1,), (1,)), ((), ())), preferred_element_type=f32)
            sc = sc + jnp.dot(qr, rope[slot], preferred_element_type=f32)
            ok = lane < count
            live.append(ok)
            parts.append(jnp.where(ok, sc * softmax_scale, floor_score))
        top = functools.reduce(jnp.maximum, parts)
        top = jnp.max(top, axis=1, keepdims=True).astype(bf16).astype(f32)
        ws = [jnp.where(o, jnp.exp(s - top), 0.0) for o, s in zip(live, parts)]
        total = jnp.sum(ws[0] + ws[1] + ws[2] + ws[3], axis=1, keepdims=True)
        w = jnp.concatenate([v.astype(bf16) for v in ws], axis=1)
        mixed = jnp.dot(w, jnp.concatenate(pages, axis=0), preferred_element_type=f32)
        full = jnp.concatenate([mixed.astype(bf16), stats(top, total)], axis=1)
        full = full.reshape(n, heads, lat_w + STAT)
        if par == 0:
            PB[0, yy] = full
        else:
            PB[1, :, yy] = full

        @pl.when(c == 1 - par)
        def _():
            part = PB.at[0, yy] if par == 0 else PB.at[1, :, yy]
            dst = RB.at[yy] if par == 0 else RB.at[:, yy]
            rcopy(part, dst, p_send.at[yy], p_recv.at[yy], sib).start()

    def stats(top, total):
        hi = total.astype(bf16)
        lo = (total - hi.astype(f32)).astype(bf16)
        lane = lax.broadcasted_iota(jnp.int32, (top.shape[0], STAT), 1)
        st = jnp.where(lane == 0, top, jnp.where(lane == 1, hi.astype(f32), lo.astype(f32)))
        return st.astype(bf16)

    def merge(values):
        tops, totals, mixes = [], [], []
        for v in values:
            st = v[:, lat_w:].astype(f32)
            tops.append(st[:, 0:1])
            totals.append(st[:, 1:2] + st[:, 2:3])
            mixes.append(v[:, :lat_w].astype(f32))
        top = functools.reduce(jnp.maximum, tops)
        fac = [jnp.exp(t - top) for t in tops]
        total = sum(f * t for f, t in zip(fac, totals))
        mixed = sum(f * m for f, m in zip(fac, mixes))
        return top, total, mixed

    def packed(top, total, mixed):
        return jnp.concatenate([mixed.astype(bf16), stats(top, total)], axis=1)

    ring_step(1)
    rcopy(TB.at[1 - c], TB.at[1 - c], td_send.at[0], td_recv.at[0], sib).wait_recv()
    build_table()
    cl.wait()
    cr.wait()
    d2d_wait(0)
    compute(0, y)
    for k in range(2, half + 1):
        ring_step(k)
        d2d_wait(k - 1)

        def pair(i, carry, k=k):
            compute(0, (y + n + (2 * i - 1) * (k - 1)) % n)
            return carry

        lax.fori_loop(0, 2, pair, 0)
    d2d_wait(half)
    compute(0, (y + half) % n)

    def odd(i, carry):
        compute(1, i)
        return carry

    lax.fori_loop(0, n, odd, 0)

    for i in range(n):
        rcopy(RB.at[i], RB.at[i], p_send.at[i], p_recv.at[i], sib).wait_recv()

    rows = half * heads

    def rslices(idx, h):
        s = pl.ds(h * half, half)
        return [PB[c, idx, s].reshape(rows, -1), RB[idx, s].reshape(rows, -1)]

    def ring_send(d, i, values):
        MS[d, i] = packed(*merge(values)).reshape(half, heads, -1)
        send(MS.at[d, i], RR.at[d, i], r_send.at[d, i], r_recv.at[d, i], nxt[d])

    def ring_recv(d, i):
        rcopy(RR.at[d, i], RR.at[d, i], r_send.at[d, i], r_recv.at[d, i], sib).wait_recv()
        return RR[d, i].reshape(rows, -1)

    def goal(d, k):
        return (b + k) % n if d == 0 else (b + n - k) % n

    for d in range(2):
        ring_send(d, 0, rslices(goal(d, half), d))
    for d in range(2):
        h = 1 - d
        ring_send(d, 1 + h, rslices(goal(d, half - 1), h))
    for d in range(2):
        ring_send(d, 1 + d, rslices(goal(d, half - 1), d) + [ring_recv(d, 0)])
    for k in range(3, half + 1):
        for j in range(2):
            for d in range(2):
                h = 1 - d if j == 0 else d
                i = 1 + 2 * (k - 2) + h
                ring_send(d, i, rslices(goal(d, half + 1 - k), h) + [ring_recv(d, i - 2)])
    for h in range(2):
        i = 1 + 2 * (half - 2) + h
        vals = rslices(b, h) + [ring_recv(0, i), ring_recv(1, i)]
        M2[pl.ds(h * half, half)] = packed(*merge(vals)).reshape(half, heads, -1)
    for k in far:
        o = (a + k) % n
        send(M2.at[o], FB.at[k], f_send.at[k], f_recv.at[k], dev_a(o))
    vals = [M2[a]]
    for k in far:
        rcopy(FB.at[k], FB.at[k], f_send.at[k], f_recv.at[k], sib).wait_recv()
        vals.append(FB[k])
    top, total, mixed = merge(vals)
    out_ref[...] = (mixed / total).astype(bf16)

    for cp in sends:
        cp.wait_send()
    for i in range(n):
        rcopy(RB.at[i], RB.at[i], p_send.at[i], p_recv.at[i], sib).wait_send()


def on_device(n, q_latent, q_rope, cache_latent, cache_rope, page_table, lengths):
    heads, lat_w = q_latent.shape[1:]
    rope_w = q_rope.shape[2]
    slots, page, _ = cache_latent.shape
    width = lat_w + STAT
    q = jnp.concatenate(
        [q_latent[0], q_rope[0], jnp.zeros((heads, width - lat_w - rope_w), bf16)], axis=1
    )
    maxp = page_table.shape[1]
    left = jnp.clip(lengths[0] - jnp.arange(maxp, dtype=jnp.int32) * page, 0, page)
    codes = jnp.where(page_table[0] >= 0, page_table[0] * 256 + left, -1).reshape(maxp // 128, 128)
    codes = jnp.concatenate([codes, jnp.full((8 - maxp // 128, 128), -1, jnp.int32)], axis=0)
    half = n // 2
    any_spec = pl.BlockSpec(memory_space=pl.ANY)
    dma = pltpu.SemaphoreType.DMA
    out = pl.pallas_call(
        functools.partial(kernel, n, heads, lat_w, rope_w, page, slots),
        out_shape=jax.ShapeDtypeStruct((heads, lat_w), bf16),
        in_specs=[any_spec] * 4,
        out_specs=pl.BlockSpec(memory_space=pltpu.VMEM),
        scratch_shapes=[
            pltpu.VMEM(cache_latent.shape, bf16),
            pltpu.VMEM(cache_rope.shape, bf16),
            pltpu.VMEM((2, n, n, heads, width), bf16),
            pltpu.VMEM((2, n, 8, 128), jnp.int32),
            pltpu.VMEM((2, n, n, heads, width), bf16),
            pltpu.VMEM((n, n, heads, width), bf16),
            pltpu.VMEM((2, n - 1, half, heads, width), bf16),
            pltpu.VMEM((2, n - 1, half, heads, width), bf16),
            pltpu.VMEM((n, heads, width), bf16),
            pltpu.VMEM((n, heads, width), bf16),
            pltpu.VMEM((8, 128), jnp.int32),
            pltpu.SMEM((8, 128), jnp.int32),
            dma((5,)),
            dma((n,)), dma((n,)), dma((n,)), dma((n,)),
            dma((2, n - 1)), dma((2, n - 1)),
            dma((2 * n - 1,)), dma((2 * n - 1,)),
            dma((1,)), dma((1,)),
            dma((n,)), dma((n,)),
            dma((2, n - 1)), dma((2, n - 1)),
            dma((n,)), dma((n,)),
        ],
        compiler_params=pltpu.CompilerParams(
            collective_id=0, has_side_effects=True, vmem_limit_bytes=48 * 1024 * 1024
        ),
    )(q, codes, cache_latent, cache_rope)
    return out[None]


def solution(mesh):
    n = mesh.shape["head"]
    assert mesh.shape["seq"] == 2 * n and n % 2 == 0
    placed = (
        P(("grp", "seq"), "head", None),
        P(("grp", "seq"), "head", None),
        P(("grp", "seq", "head"), None, None),
        P(("grp", "seq", "head"), None, None),
        P(("grp", "seq"), None),
        P(("grp", "seq")),
    )
    return jax.shard_map(
        functools.partial(on_device, n),
        mesh=mesh,
        in_specs=placed,
        out_specs=P(("grp", "seq"), "head", None),
        check_vma=False,
    )
```

```python
import functools

import jax
import jax.numpy as jnp
from jax import lax
from jax.experimental import pallas as pl
from jax.experimental.pallas import tpu as pltpu
from jax.sharding import PartitionSpec as P

softmax_scale = 0.13528
floor_score = -1e30
MESH = pl.DeviceIdType.MESH
MOST = 4
STAT = 128
SUBS = 4
bf16, f32 = jnp.bfloat16, jnp.float32


def kernel(
    n, heads, lat_w, rope_w, page, slots,
    ql_hbm, qr_hbm, lat_hbm, rope_hbm, pt_hbm, len_ref,
    out_ref,
    lat, rope, QB, TB, SB, RB, LM, LT, LS, RR, MS, M2, FB, qrv, ptv, tvm, tsm,
    loc, a_send, a_recv, t_send, t_recv, g_send, g_recv, d_send, d_recv, td_send, td_recv,
    p_send, p_recv, r_send, r_recv, f_send, f_recv,
):
    half = n // 2
    per = n // SUBS
    lanes = lat_w // 128
    sq = lax.axis_index("seq")
    x = lax.axis_index("head")
    y = sq // 2
    c = sq % 2
    a = x * (1 - c) + y * c
    b = y * (1 - c) + x * c

    def at(xx, yy, cc):
        return {"seq": 2 * yy + cc, "head": xx}

    def dev_a(i):
        return at(i * (1 - c) + x * c, y * (1 - c) + i * c, c)

    def dev_b(i):
        return at(x * (1 - c) + i * c, i * (1 - c) + y * c, c)

    sib = at(x, y, 1 - c)

    def rcopy(src, dst, ss, rs, dev):
        return pltpu.make_async_remote_copy(
            src_ref=src, dst_ref=dst, send_sem=ss, recv_sem=rs, device_id=dev, device_id_type=MESH
        )

    sends = []

    def send(src, dst, ss, rs, dev):
        cp = rcopy(src, dst, ss, rs, dev)
        cp.start()
        sends.append(cp)

    bar = pltpu.get_barrier_semaphore()
    far = sorted(range(1, n), key=lambda k: -min(k, n - k))
    for k in far:
        pl.semaphore_signal(bar, inc=1, device_id=dev_a((a + k) % n), device_id_type=MESH)
        pl.semaphore_signal(bar, inc=1, device_id=dev_b((b + k) % n), device_id_type=MESH)
    pl.semaphore_signal(bar, inc=1, device_id=sib, device_id_type=MESH)

    own = QB.at[c, b, a]
    cq = pltpu.make_async_copy(ql_hbm.at[0], own.at[:, pl.ds(0, lat_w)], loc.at[0])
    cs = pltpu.make_async_copy(qr_hbm.at[0], qrv, loc.at[1])
    ct = pltpu.make_async_copy(pt_hbm, ptv, loc.at[2])
    cl = pltpu.make_async_copy(lat_hbm, lat, loc.at[3])
    cr = pltpu.make_async_copy(rope_hbm, rope, loc.at[4])
    cq.start()
    cs.start()
    ct.start()
    cl.start()
    cr.start()

    ct.wait()
    rows_t = []
    lane1 = lax.broadcasted_iota(jnp.int32, (1, 128), 1)
    entries = ptv.shape[1] // 128
    for r in range(entries):
        v = ptv[:, r * 128 : (r + 1) * 128]
        live = jnp.clip(len_ref[0] - (lane1 + r * 128) * page, 0, page)
        rows_t.append(jnp.where(v >= 0, v * 256 + live, -1))
    rows_t.append(jnp.full((8 - entries, 128), -1, jnp.int32))
    TB[c, y] = jnp.concatenate(rows_t, axis=0)
    cs.wait()
    QB[c, b, a, :, pl.ds(lat_w, STAT)] = jnp.concatenate(
        [qrv[...], jnp.zeros((heads, STAT - rope_w), bf16)], axis=1
    )
    cq.wait()

    pl.semaphore_wait(bar, 2 * (n - 1) + 1)

    for k in far:
        send(own, own, a_send.at[k], a_recv.at[k], dev_a((a + k) % n))
    for k in far:
        send(TB.at[c, y], TB.at[c, y], t_send.at[k], t_recv.at[k], at(x, (y + k) % n, c))
    for k in far:
        part = QB.at[c, b, (a + n - k) % n]
        rcopy(part, part, a_send.at[k], a_recv.at[k], sib).wait_recv()

    def gpart(idx, j):
        return QB.at[c, idx, pl.ds(j * per, per)]

    right, left = dev_b((b + 1) % n), dev_b((b + n - 1) % n)
    nxt = (right, left)
    order = (
        tuple(range(SUBS)),
        tuple(range(SUBS // 2, SUBS)) + tuple(range(SUBS // 2)),
    )
    own_i = 2 * (half * SUBS)

    for j in range(SUBS):
        for d in range(2):
            p = order[d][j]
            send(gpart(b, p), gpart(b, p), g_send.at[d, p], g_recv.at[d, p], nxt[d])
    send(QB.at[c, b], QB.at[c, b], d_send.at[own_i], d_recv.at[own_i], sib)

    for k in far:
        part = TB.at[c, (y + n - k) % n]
        rcopy(part, part, t_send.at[k], t_recv.at[k], sib).wait_recv()
    send(TB.at[c], TB.at[c], td_send.at[0], td_recv.at[0], sib)

    def ring_sub(k, j):
        if k == half and j >= SUBS // 2:
            return
        for d in range(2):
            p = order[d][j]
            o = (b + n - k) % n if d == 0 else (b + k) % n
            i = (k - 1) * SUBS + p
            part = gpart(o, p)
            rcopy(part, part, g_send.at[d, i], g_recv.at[d, i], sib).wait_recv()
            if k < half - 1 or (k == half - 1 and j < SUBS // 2):
                send(part, part, g_send.at[d, i + SUBS], g_recv.at[d, i + SUBS], nxt[d])
            dd = d * half * SUBS + i
            send(part, part, d_send.at[dd], d_recv.at[dd], sib)

    b_sib = y * c + x * (1 - c)

    def d2d_wait(k):
        if k == 0:
            part = QB.at[1 - c, b_sib]
            rcopy(part, part, d_send.at[own_i], d_recv.at[own_i], sib).wait_recv()
            return
        for j in range(SUBS if k < half else SUBS // 2):
            for d in range(2):
                p = order[d][j]
                o = (b_sib + n - k) % n if d == 0 else (b_sib + k) % n
                dd = d * half * SUBS + (k - 1) * SUBS + p
                part = QB.at[1 - c, o, pl.ds(p * per, per)]
                rcopy(part, part, d_send.at[dd], d_recv.at[dd], sib).wait_recv()

    def build_table():
        first = (sq * n + x) * slots * 256
        codes = TB[...].reshape(n * 16, 128)
        ok = (codes >= first) & (codes < first + slots * 256)
        key = jnp.where(ok, codes - first, -1).T
        row = lax.broadcasted_iota(jnp.int32, (8, 128), 0)
        lane = lax.broadcasted_iota(jnp.int32, (8, 128), 1)
        res = jnp.full((8, 128), -1, jnp.int32)
        for j in range(MOST):
            m = key
            size = key.shape[0]
            while size > 8:
                size //= 2
                m = jnp.maximum(m[:size], m[size:])
            for r in (4, 2, 1):
                m = jnp.maximum(m, pltpu.roll(m, r, 0))
            for bit in (1, 2, 4):
                other = jnp.where(
                    (lane & bit) > 0, pltpu.roll(m, bit, 1), pltpu.roll(m, 128 - bit, 1)
                )
                m = jnp.maximum(m, other)
            res = jnp.where(row == j, m, res)
            key = jnp.where(key == jnp.concatenate([m] * (n * 2), axis=0), -1, key)
        tvm[...] = res
        cp = pltpu.make_async_copy(tvm, tsm, loc.at[5])
        cp.start()
        cp.wait()

    def stats(top, total):
        hi = total.astype(bf16)
        lo = (total - hi.astype(f32)).astype(bf16)
        lane = lax.broadcasted_iota(jnp.int32, top.shape, 1)
        st = jnp.where(lane == 0, top, jnp.where(lane == 1, hi.astype(f32), lo.astype(f32)))
        return st.astype(bf16)

    def compute(par, yy):
        q = (QB[0, yy] if par == 0 else QB[1, :, yy]).reshape(n * heads, -1)
        ql, qr = q[:, :lat_w], q[:, lat_w : lat_w + rope_w]
        pages, ropes, counts = [], [], []
        for j in range(MOST):
            code = tsm[j, 8 * (par * n + yy)]
            slot = jnp.maximum(code, 0) // 256
            counts.append(jnp.where(code < 0, 0, code % 256))
            pages.append(lat[slot])
            ropes.append(rope[slot])
        keys = jnp.concatenate(pages, axis=0)
        sc = lax.dot_general(ql, keys, (((1,), (1,)), ((), ())), preferred_element_type=f32)
        sc = sc + jnp.dot(qr, jnp.concatenate(ropes, axis=1), preferred_element_type=f32)
        lane = lax.broadcasted_iota(jnp.int32, (n * heads, page), 1)
        live = [lane < v for v in counts]
        parts = [
            jnp.where(live[j], sc[:, j * page : (j + 1) * page] * softmax_scale, floor_score)
            for j in range(MOST)
        ]
        top = functools.reduce(jnp.maximum, parts)
        top = jnp.max(top, axis=1, keepdims=True).astype(bf16).astype(f32)
        ws = [jnp.where(o, jnp.exp(s - top), 0.0) for o, s in zip(live, parts)]
        total = jnp.sum(ws[0] + ws[1] + ws[2] + ws[3], axis=1, keepdims=True)
        w = jnp.concatenate([v.astype(bf16) for v in ws], axis=1)
        mixed = jnp.dot(w, keys, preferred_element_type=f32)
        top = jnp.broadcast_to(top, (n * heads, STAT))
        total = jnp.broadcast_to(total, (n * heads, STAT))
        shape = (n, heads, -1)

        @pl.when(c == par)
        def _():
            if par == 0:
                LM[yy] = mixed.reshape(shape)
                LT[yy] = top.reshape(shape)
                LS[yy] = total.reshape(shape)
            else:
                LM[:, yy] = mixed.reshape(shape)
                LT[:, yy] = top.reshape(shape)
                LS[:, yy] = total.reshape(shape)

        @pl.when(c == 1 - par)
        def _():
            full = jnp.concatenate([mixed.astype(bf16), stats(top, total)], axis=1)
            SB[yy] = full.reshape(shape)
            dst = RB.at[yy] if par == 0 else RB.at[:, yy]
            rcopy(SB.at[yy], dst, p_send.at[yy], p_recv.at[yy], sib).start()

    for j in range(SUBS):
        ring_sub(1, j)
    rcopy(TB.at[1 - c], TB.at[1 - c], td_send.at[0], td_recv.at[0], sib).wait_recv()
    build_table()
    cl.wait()
    cr.wait()
    d2d_wait(0)
    compute(0, y)
    for k in range(2, half + 1):
        for j in range(SUBS // 2):
            ring_sub(k, j)
        d2d_wait(k - 1)
        compute(0, (y + n - (k - 1)) % n)
        for j in range(SUBS // 2, SUBS):
            ring_sub(k, j)
        compute(0, (y + k - 1) % n)
    d2d_wait(half)
    compute(0, (y + half) % n)

    def odd(i, carry):
        compute(1, i)
        return carry

    lax.fori_loop(0, n, odd, 0)

    rows = half * heads
    er = lax.broadcasted_iota(jnp.int32, (STAT, 2 * STAT), 0)
    ec = lax.broadcasted_iota(jnp.int32, (STAT, 2 * STAT), 1)
    spread = jnp.where(
        ((er == 0) & (ec < STAT)) | ((er > 0) & (er < 3) & (ec >= STAT)), 1.0, 0.0
    ).astype(bf16)

    def opened(v):
        s = jnp.dot(v[:, lat_w:], spread, preferred_element_type=f32)
        tiles = [v[:, j * 128 : (j + 1) * 128].astype(f32) for j in range(lanes)]
        return tiles, s[:, :STAT], s[:, STAT:]

    def merge(states):
        top = functools.reduce(jnp.maximum, [s[1] for s in states])
        fac = [jnp.exp(s[1] - top) for s in states]
        total = sum(f * s[2] for f, s in zip(fac, states))
        tiles = [sum(f * s[0][j] for f, s in zip(fac, states)) for j in range(lanes)]
        return tiles, top, total

    def packed(state):
        tiles, top, total = state
        return jnp.concatenate([t.astype(bf16) for t in tiles] + [stats(top, total)], axis=1)

    def hs(h):
        return pl.ds(h * half, half)

    def local(idx, h):
        v = LM[idx, hs(h)].reshape(rows, lat_w)
        tiles = [v[:, j * 128 : (j + 1) * 128] for j in range(lanes)]
        return tiles, LT[idx, hs(h)].reshape(rows, STAT), LS[idx, hs(h)].reshape(rows, STAT)

    def both(idx, h):
        return merge([local(idx, h), opened(RB[idx, hs(h)].reshape(rows, -1))])

    def premerge(idx, h):
        tiles, top, total = both(idx, h)
        LM[idx, hs(h)] = jnp.concatenate(tiles, axis=1).reshape(half, heads, lat_w)
        LT[idx, hs(h)] = top.reshape(half, heads, STAT)
        LS[idx, hs(h)] = total.reshape(half, heads, STAT)

    def ring_send(d, i, state):
        MS[d, i] = packed(state).reshape(half, heads, -1)
        send(MS.at[d, i], RR.at[d, i], r_send.at[d, i], r_recv.at[d, i], nxt[d])

    def ring_recv(d, i):
        rcopy(RR.at[d, i], RR.at[d, i], r_send.at[d, i], r_recv.at[d, i], sib).wait_recv()
        return opened(RR[d, i].reshape(rows, -1))

    def goal(d, k):
        return (b + k) % n if d == 0 else (b + n - k) % n

    for i in range(n):
        rcopy(RB.at[i], RB.at[i], p_send.at[i], p_recv.at[i], sib).wait_recv()

    for d in range(2):
        ring_send(d, 0, both(goal(d, half), d))
    for d in range(2):
        ring_send(d, 2 - d, both(goal(d, half - 1), 1 - d))
    for d in range(2):
        premerge(goal(d, half - 1), d)

    def pre(i, carry):
        idx = (b + n - (half - 2) + i // 2) % n
        premerge(idx, i % 2)
        return carry

    lax.fori_loop(0, 2 * (2 * (half - 2) + 1), pre, 0)

    for d in range(2):
        ring_send(d, 1 + d, merge([local(goal(d, half - 1), d), ring_recv(d, 0)]))
    for k in range(3, half + 1):
        for j in range(2):
            for d in range(2):
                h = 1 - d if j == 0 else d
                i = 1 + 2 * (k - 2) + h
                ring_send(d, i, merge([local(goal(d, half + 1 - k), h), ring_recv(d, i - 2)]))
    for h in range(2):
        i = 1 + 2 * (half - 2) + h
        state = merge([local(b, h), ring_recv(0, i), ring_recv(1, i)])
        M2[hs(h)] = packed(state).reshape(half, heads, -1)
    for k in far:
        o = (a + k) % n
        send(M2.at[o], FB.at[k], f_send.at[k], f_recv.at[k], dev_a(o))
    states = [opened(M2[a])]
    for k in far:
        rcopy(FB.at[k], FB.at[k], f_send.at[k], f_recv.at[k], sib).wait_recv()
        states.append(opened(FB[k]))
    tiles, top, total = merge(states)
    out_ref[...] = jnp.concatenate([(t / total).astype(bf16) for t in tiles], axis=1)

    for cp in sends:
        cp.wait_send()
    for i in range(n):
        rcopy(SB.at[i], SB.at[i], p_send.at[i], p_recv.at[i], sib).wait_send()


def on_device(n, q_latent, q_rope, cache_latent, cache_rope, page_table, lengths):
    heads, lat_w = q_latent.shape[1:]
    rope_w = q_rope.shape[2]
    slots, page, _ = cache_latent.shape
    width = lat_w + STAT
    half = n // 2
    any_spec = pl.BlockSpec(memory_space=pl.ANY)
    dma = pltpu.SemaphoreType.DMA
    out = pl.pallas_call(
        functools.partial(kernel, n, heads, lat_w, rope_w, page, slots),
        out_shape=jax.ShapeDtypeStruct((heads, lat_w), bf16),
        in_specs=[any_spec] * 5 + [pl.BlockSpec(memory_space=pltpu.SMEM)],
        out_specs=pl.BlockSpec(memory_space=pltpu.VMEM),
        scratch_shapes=[
            pltpu.VMEM(cache_latent.shape, bf16),
            pltpu.VMEM(cache_rope.shape, bf16),
            pltpu.VMEM((2, n, n, heads, width), bf16),
            pltpu.VMEM((2, n, 8, 128), jnp.int32),
            pltpu.VMEM((n, n, heads, width), bf16),
            pltpu.VMEM((n, n, heads, width), bf16),
            pltpu.VMEM((n, n, heads, lat_w), f32),
            pltpu.VMEM((n, n, heads, STAT), f32),
            pltpu.VMEM((n, n, heads, STAT), f32),
            pltpu.VMEM((2, n - 1, half, heads, width), bf16),
            pltpu.VMEM((2, n - 1, half, heads, width), bf16),
            pltpu.VMEM((n, heads, width), bf16),
            pltpu.VMEM((n, heads, width), bf16),
            pltpu.VMEM((heads, rope_w), bf16),
            pltpu.VMEM(page_table.shape, jnp.int32),
            pltpu.VMEM((8, 128), jnp.int32),
            pltpu.SMEM((8, 128), jnp.int32),
            dma((6,)),
            dma((n,)), dma((n,)), dma((n,)), dma((n,)),
            dma((2, half * SUBS)), dma((2, half * SUBS)),
            dma((2 * half * SUBS + 1,)), dma((2 * half * SUBS + 1,)),
            dma((1,)), dma((1,)),
            dma((n,)), dma((n,)),
            dma((2, n - 1)), dma((2, n - 1)),
            dma((n,)), dma((n,)),
        ],
        compiler_params=pltpu.CompilerParams(
            collective_id=0, has_side_effects=True, vmem_limit_bytes=57 * 1024 * 1024
        ),
    )(q_latent, q_rope, cache_latent, cache_rope, page_table, lengths)
    return out[None]


def solution(mesh):
    n = mesh.shape["head"]
    assert mesh.shape["seq"] == 2 * n and n % 2 == 0
    placed = (
        P(("grp", "seq"), "head", None),
        P(("grp", "seq"), "head", None),
        P(("grp", "seq", "head"), None, None),
        P(("grp", "seq", "head"), None, None),
        P(("grp", "seq"), None),
        P(("grp", "seq")),
    )
    return jax.shard_map(
        functools.partial(on_device, n),
        mesh=mesh,
        in_specs=placed,
        out_specs=P(("grp", "seq"), "head", None),
        check_vma=False,
    )
```

```python
import functools

import jax
import jax.numpy as jnp
from jax import lax
from jax.experimental import pallas as pl
from jax.experimental.pallas import tpu as pltpu
from jax.sharding import PartitionSpec as P

softmax_scale = 0.13528
floor_score = -1e30
MESH = pl.DeviceIdType.MESH
MOST = 4
STAT = 128
SUBS = 4
bf16, f32 = jnp.bfloat16, jnp.float32


def kernel(
    n, heads, lat_w, rope_w, page, slots,
    ql_hbm, qr_hbm, lat_hbm, rope_hbm, pt_hbm, len_ref,
    out_ref,
    lat, rope, QB, TB, SB, RB, LM, LT, LS, RR, MS, M2, FB, qown, town, qrv, ptv, tvm, tsm,
    loc, a_send, a_recv, t_send, t_recv, g_send, g_recv, d_send, d_recv, o_send, o_recv,
    p_send, p_recv, r_send, r_recv, f_send, f_recv,
):
    half = n // 2
    per = n // SUBS
    lanes = lat_w // 128
    sq = lax.axis_index("seq")
    x = lax.axis_index("head")
    y = sq // 2
    c = sq % 2
    a = x * (1 - c) + y * c
    b = y * (1 - c) + x * c

    def at(xx, yy, cc):
        return {"seq": 2 * yy + cc, "head": xx}

    def dev_a(i):
        return at(i * (1 - c) + x * c, y * (1 - c) + i * c, c)

    def dev_b(i):
        return at(x * (1 - c) + i * c, i * (1 - c) + y * c, c)

    sib = at(x, y, 1 - c)

    def rcopy(src, dst, ss, rs, dev):
        return pltpu.make_async_remote_copy(
            src_ref=src, dst_ref=dst, send_sem=ss, recv_sem=rs, device_id=dev, device_id_type=MESH
        )

    sends = []

    def send(src, dst, ss, rs, dev):
        cp = rcopy(src, dst, ss, rs, dev)
        cp.start()
        sends.append(cp)

    bar = pltpu.get_barrier_semaphore()
    far = sorted(range(1, n), key=lambda k: -min(k, n - k))
    partners = [at((x + k) % n, y, 1 - c) for k in far]
    partners += [at(x, (y + k) % n, 1 - c) for k in far]
    partners += [dev_a((a + k) % n) for k in far]
    partners += [dev_b((b + 1) % n), dev_b((b + n - 1) % n), sib]
    for dev in partners:
        pl.semaphore_signal(bar, inc=1, device_id=dev, device_id_type=MESH)

    cq = pltpu.make_async_copy(ql_hbm.at[0], qown.at[:, pl.ds(0, lat_w)], loc.at[0])
    cs = pltpu.make_async_copy(qr_hbm.at[0], qrv, loc.at[1])
    ct = pltpu.make_async_copy(pt_hbm, ptv, loc.at[2])
    cl = pltpu.make_async_copy(lat_hbm, lat, loc.at[3])
    cr = pltpu.make_async_copy(rope_hbm, rope, loc.at[4])
    ct.start()
    cs.start()
    cq.start()
    cl.start()
    cr.start()

    ct.wait()
    rows_t = []
    lane1 = lax.broadcasted_iota(jnp.int32, (1, 128), 1)
    entries = ptv.shape[1] // 128
    for r in range(entries):
        v = ptv[:, r * 128 : (r + 1) * 128]
        live = jnp.clip(len_ref[0] - (lane1 + r * 128) * page, 0, page)
        rows_t.append(jnp.where(v >= 0, v * 256 + live, -1))
    rows_t.append(jnp.full((8 - entries, 128), -1, jnp.int32))
    town[...] = jnp.concatenate(rows_t, axis=0)
    cs.wait()
    qown[:, pl.ds(lat_w, STAT)] = jnp.concatenate(
        [qrv[...], jnp.zeros((heads, STAT - rope_w), bf16)], axis=1
    )
    cq.wait()

    pl.semaphore_wait(bar, len(partners))

    for k in far:
        dev = at((x + k * (1 - c)) % n, (y + k * c) % n, 1)
        send(qown, QB.at[c, b, a], a_send.at[k], a_recv.at[c, k], dev)
    for k in far:
        send(town, TB.at[c, y], t_send.at[k], t_recv.at[c, k], at(x, (y + k) % n, 1))

    def part_of(par, idx, p):
        return QB.at[par, idx, pl.ds(p * per, per)]

    order = (
        tuple(range(SUBS)),
        tuple(range(SUBS // 2, SUBS)) + tuple(range(SUBS // 2)),
    )
    mid = (y, x)

    def origin(par, d, k):
        return (mid[par] + n - k) % n if d == 0 else (mid[par] + k) % n

    def subs_at(k):
        return SUBS // 2 if k == half else SUBS

    def build_table():
        first = (sq * n + x) * slots * 256
        codes = TB[...].reshape(n * 16, 128)
        ok = (codes >= first) & (codes < first + slots * 256)
        key = jnp.where(ok, codes - first, -1).T
        row = lax.broadcasted_iota(jnp.int32, (8, 128), 0)
        lane = lax.broadcasted_iota(jnp.int32, (8, 128), 1)
        res = jnp.full((8, 128), -1, jnp.int32)
        for j in range(MOST):
            m = key
            size = key.shape[0]
            while size > 8:
                size //= 2
                m = jnp.maximum(m[:size], m[size:])
            for r in (4, 2, 1):
                m = jnp.maximum(m, pltpu.roll(m, r, 0))
            for bit in (1, 2, 4):
                other = jnp.where(
                    (lane & bit) > 0, pltpu.roll(m, bit, 1), pltpu.roll(m, 128 - bit, 1)
                )
                m = jnp.maximum(m, other)
            res = jnp.where(row == j, m, res)
            key = jnp.where(key == jnp.concatenate([m] * (n * 2), axis=0), -1, key)
        tvm[...] = res
        cp = pltpu.make_async_copy(tvm, tsm, loc.at[5])
        cp.start()
        cp.wait()

    def stats(top, total):
        hi = total.astype(bf16)
        lo = (total - hi.astype(f32)).astype(bf16)
        lane = lax.broadcasted_iota(jnp.int32, top.shape, 1)
        st = jnp.where(lane == 0, top, jnp.where(lane == 1, hi.astype(f32), lo.astype(f32)))
        return st.astype(bf16)

    def compute(par, yy, own):
        q = (QB[0, yy] if par == 0 else QB[1, :, yy]).reshape(n * heads, -1)
        ql, qr = q[:, :lat_w], q[:, lat_w : lat_w + rope_w]
        pages, ropes, counts = [], [], []
        for j in range(MOST):
            code = tsm[j, 8 * (par * n + yy)]
            slot = jnp.maximum(code, 0) // 256
            counts.append(jnp.where(code < 0, 0, code % 256))
            pages.append(lat[slot])
            ropes.append(rope[slot])
        keys = jnp.concatenate(pages, axis=0)
        sc = lax.dot_general(ql, keys, (((1,), (1,)), ((), ())), preferred_element_type=f32)
        sc = sc + jnp.dot(qr, jnp.concatenate(ropes, axis=1), preferred_element_type=f32)
        lane = lax.broadcasted_iota(jnp.int32, (n * heads, page), 1)
        live = [lane < v for v in counts]
        parts = [
            jnp.where(live[j], sc[:, j * page : (j + 1) * page] * softmax_scale, floor_score)
            for j in range(MOST)
        ]
        top = functools.reduce(jnp.maximum, parts)
        top = jnp.max(top, axis=1, keepdims=True).astype(bf16).astype(f32)
        ws = [jnp.where(o, jnp.exp(s - top), 0.0) for o, s in zip(live, parts)]
        total = jnp.sum(ws[0] + ws[1] + ws[2] + ws[3], axis=1, keepdims=True)
        w = jnp.concatenate([v.astype(bf16) for v in ws], axis=1)
        mixed = jnp.dot(w, keys, preferred_element_type=f32)
        top = jnp.broadcast_to(top, (n * heads, STAT))
        total = jnp.broadcast_to(total, (n * heads, STAT))
        shape = (n, heads, -1)

        if own and par == 0:
            LM[yy] = mixed.reshape(shape)
            LT[yy] = top.reshape(shape)
            LS[yy] = total.reshape(shape)
        elif own:
            LM[:, yy] = mixed.reshape(shape)
            LT[:, yy] = top.reshape(shape)
            LS[:, yy] = total.reshape(shape)
        else:
            full = jnp.concatenate([mixed.astype(bf16), stats(top, total)], axis=1)
            SB[yy] = full.reshape(shape)
            dst = RB.at[yy] if par == 0 else RB.at[:, yy]
            rcopy(SB.at[yy], dst, p_send.at[yy], p_recv.at[yy], sib).start()

    rows = half * heads
    er = lax.broadcasted_iota(jnp.int32, (STAT, 2 * STAT), 0)
    ec = lax.broadcasted_iota(jnp.int32, (STAT, 2 * STAT), 1)
    spread = jnp.where(
        ((er == 0) & (ec < STAT)) | ((er > 0) & (er < 3) & (ec >= STAT)), 1.0, 0.0
    ).astype(bf16)

    def opened(v):
        s = jnp.dot(v[:, lat_w:], spread, preferred_element_type=f32)
        tiles = [v[:, j * 128 : (j + 1) * 128].astype(f32) for j in range(lanes)]
        return tiles, s[:, :STAT], s[:, STAT:]

    def merge(states):
        top = functools.reduce(jnp.maximum, [s[1] for s in states])
        fac = [jnp.exp(s[1] - top) for s in states]
        total = sum(f * s[2] for f, s in zip(fac, states))
        tiles = [sum(f * s[0][j] for f, s in zip(fac, states)) for j in range(lanes)]
        return tiles, top, total

    def packed(state):
        tiles, top, total = state
        return jnp.concatenate([t.astype(bf16) for t in tiles] + [stats(top, total)], axis=1)

    def hs(h):
        return pl.ds(h * half, half)

    def local(idx, h):
        v = LM[idx, hs(h)].reshape(rows, lat_w)
        tiles = [v[:, j * 128 : (j + 1) * 128] for j in range(lanes)]
        return tiles, LT[idx, hs(h)].reshape(rows, STAT), LS[idx, hs(h)].reshape(rows, STAT)

    def both(idx, h):
        return merge([local(idx, h), opened(RB[idx, hs(h)].reshape(rows, -1))])

    def premerge(idx, h):
        tiles, top, total = both(idx, h)
        LM[idx, hs(h)] = jnp.concatenate(tiles, axis=1).reshape(half, heads, lat_w)
        LT[idx, hs(h)] = top.reshape(half, heads, STAT)
        LS[idx, hs(h)] = total.reshape(half, heads, STAT)

    def goal(d, k):
        return (b + k) % n if d == 0 else (b + n - k) % n

    nxt = (dev_b((b + 1) % n), dev_b((b + n - 1) % n))

    def reduce(gaps):
        out = []

        def put(src, dst, ss, rs, dev):
            cp = rcopy(src, dst, ss, rs, dev)
            cp.start()
            out.append(cp)

        def ring_send(d, i, state):
            MS[d, i] = packed(state).reshape(half, heads, -1)
            put(MS.at[d, i], RR.at[d, i], r_send.at[d, i], r_recv.at[d, i], nxt[d])

        def ring_recv(d, i):
            rcopy(RR.at[d, i], RR.at[d, i], r_send.at[d, i], r_recv.at[d, i], sib).wait_recv()
            return opened(RR[d, i].reshape(rows, -1))

        def pre(k):
            for d in range(2 if k else 1):
                for h in range(2):
                    premerge(goal(d, k), h)

        for i in range(n):
            rcopy(RB.at[i], RB.at[i], p_send.at[i], p_recv.at[i], sib).wait_recv()
        for d in range(2):
            ring_send(d, 0, both(goal(d, half), d))
        for d in range(2):
            ring_send(d, 2 - d, both(goal(d, half - 1), 1 - d))
        for d in range(2):
            premerge(goal(d, half - 1), d)
        gaps[0]()
        for d in range(2):
            ring_send(d, 1 + d, merge([local(goal(d, half - 1), d), ring_recv(d, 0)]))
        for k in range(3, half + 1):
            pre(half + 1 - k)
            gaps[k - 2]()
            for j in range(2):
                for d in range(2):
                    h = 1 - d if j == 0 else d
                    i = 1 + 2 * (k - 2) + h
                    ring_send(d, i, merge([local(goal(d, half + 1 - k), h), ring_recv(d, i - 2)]))
        pre(0)
        gaps[half - 1]()
        for h in range(2):
            i = 1 + 2 * (half - 2) + h
            state = merge([local(b, h), ring_recv(0, i), ring_recv(1, i)])
            M2[hs(h)] = packed(state).reshape(half, heads, -1)
        for k in far:
            o = (a + k) % n
            put(M2.at[o], FB.at[k], f_send.at[k], f_recv.at[k], dev_a(o))
        states = [opened(M2[a])]
        for k in far:
            rcopy(FB.at[k], FB.at[k], f_send.at[k], f_recv.at[k], sib).wait_recv()
            states.append(opened(FB[k]))
        tiles, top, total = merge(states)
        out_ref[...] = jnp.concatenate([(t / total).astype(bf16) for t in tiles], axis=1)
        for i in range(n):
            rcopy(SB.at[i], SB.at[i], p_send.at[i], p_recv.at[i], sib).wait_send()
        for cp in out:
            cp.wait_send()

    def nothing():
        return

    @pl.when(c == 1)
    def _():
        out = []

        def put(src, dst, ss, rs, dev):
            cp = rcopy(src, dst, ss, rs, dev)
            cp.start()
            out.append(cp)

        neighbour = (
            (at(x, (y + 1) % n, 1), at(x, (y + n - 1) % n, 1)),
            (at((x + 1) % n, y, 1), at((x + n - 1) % n, y, 1)),
        )
        QB[1, x, y] = qown[...]
        TB[1, y] = town[...]
        for par in (1, 0):
            for k in far + ([0] if par == 0 else []):
                src = (x + n - k) % n if par == 0 else (y + n - k) % n
                part = QB.at[par, mid[par], src]
                rcopy(part, part, a_send.at[k], a_recv.at[par, k], sib).wait_recv()
            for j in range(SUBS):
                for d in range(2):
                    p = order[d][j]
                    part = part_of(par, mid[par], p)
                    put(part, part, g_send.at[par, d, p], g_recv.at[par, d, p], neighbour[par][d])
            part = QB.at[par, mid[par]]
            put(part, part, o_send.at[par], o_recv.at[par], sib)
        for par in (1, 0):
            for k in far + ([0] if par == 0 else []):
                part = TB.at[par, (y + n - k) % n]
                rcopy(part, part, t_send.at[k], t_recv.at[par, k], sib).wait_recv()
        put(TB, TB, o_send.at[2], o_recv.at[2], sib)
        build_table()
        cl.wait()
        cr.wait()

        def ring_sub(k, j):
            for par in (1, 0):
                for d in range(2):
                    p = order[d][j]
                    i = (k - 1) * SUBS + p
                    part = part_of(par, origin(par, d, k), p)
                    rcopy(part, part, g_send.at[par, d, i], g_recv.at[par, d, i], sib).wait_recv()
                    if k < half - 1 or (k == half - 1 and j < SUBS // 2):
                        i2 = i + SUBS
                        ss, rs = g_send.at[par, d, i2], g_recv.at[par, d, i2]
                        put(part, part, ss, rs, neighbour[par][d])
                    put(part, part, d_send.at[par, d, i], d_recv.at[par, d, i], sib)

        compute(0, y, False)
        rest = [(y + half) % n]
        for k in range(half - 1, 0, -1):
            rest += [(y + n - k) % n, (y + k) % n]
        for k in range(1, half + 1):
            for j in range(subs_at(k)):
                ring_sub(k, j)
            if k < half:
                compute(0, rest.pop(), False)
        while rest:
            compute(0, rest.pop(), False)

        def odd(i, carry):
            compute(1, i, True)
            return carry

        lax.fori_loop(0, n, odd, 0)
        reduce([nothing] * half)
        for cp in out:
            cp.wait_send()

    @pl.when(c == 0)
    def _():
        put_a = rcopy(qown, QB.at[0, y, x], a_send.at[0], a_recv.at[0, 0], sib)
        put_t = rcopy(town, TB.at[0, y], t_send.at[0], t_recv.at[0, 0], sib)
        put_a.start()
        put_t.start()

        def arrived(par, k):
            if k == 0:
                part = QB.at[par, mid[par]]
                rcopy(part, part, o_send.at[par], o_recv.at[par], sib).wait_recv()
                return
            for j in range(subs_at(k)):
                for d in range(2):
                    p = order[d][j]
                    i = (k - 1) * SUBS + p
                    part = part_of(par, origin(par, d, k), p)
                    rcopy(part, part, d_send.at[par, d, i], d_recv.at[par, d, i], sib).wait_recv()

        rcopy(TB, TB, o_send.at[2], o_recv.at[2], sib).wait_recv()
        build_table()
        cl.wait()
        cr.wait()
        arrived(0, 0)
        compute(0, y, True)
        for k in range(1, half + 1):
            arrived(0, k)
            compute(0, (y + n - k) % n, True)
            if k < half:
                compute(0, (y + k) % n, True)
        for k in range(half + 1):
            arrived(1, k)

        def odds(first, last):
            def body(i, carry):
                compute(1, i, False)
                return carry

            return lambda: lax.fori_loop(first, last, body, 0) and None

        reduce([odds(0, 3 * n // 4), odds(3 * n // 4, n)] + [nothing] * (half - 2))
        put_a.wait_send()
        put_t.wait_send()

    for cp in sends:
        cp.wait_send()


def on_device(n, q_latent, q_rope, cache_latent, cache_rope, page_table, lengths):
    heads, lat_w = q_latent.shape[1:]
    rope_w = q_rope.shape[2]
    slots, page, _ = cache_latent.shape
    width = lat_w + STAT
    half = n // 2
    any_spec = pl.BlockSpec(memory_space=pl.ANY)
    dma = pltpu.SemaphoreType.DMA
    out = pl.pallas_call(
        functools.partial(kernel, n, heads, lat_w, rope_w, page, slots),
        out_shape=jax.ShapeDtypeStruct((heads, lat_w), bf16),
        in_specs=[any_spec] * 5 + [pl.BlockSpec(memory_space=pltpu.SMEM)],
        out_specs=pl.BlockSpec(memory_space=pltpu.VMEM),
        scratch_shapes=[
            pltpu.VMEM(cache_latent.shape, bf16),
            pltpu.VMEM(cache_rope.shape, bf16),
            pltpu.VMEM((2, n, n, heads, width), bf16),
            pltpu.VMEM((2, n, 8, 128), jnp.int32),
            pltpu.VMEM((n, n, heads, width), bf16),
            pltpu.VMEM((n, n, heads, width), bf16),
            pltpu.VMEM((n, n, heads, lat_w), f32),
            pltpu.VMEM((n, n, heads, STAT), f32),
            pltpu.VMEM((n, n, heads, STAT), f32),
            pltpu.VMEM((2, n - 1, half, heads, width), bf16),
            pltpu.VMEM((2, n - 1, half, heads, width), bf16),
            pltpu.VMEM((n, heads, width), bf16),
            pltpu.VMEM((n, heads, width), bf16),
            pltpu.VMEM((heads, width), bf16),
            pltpu.VMEM((8, 128), jnp.int32),
            pltpu.VMEM((heads, rope_w), bf16),
            pltpu.VMEM(page_table.shape, jnp.int32),
            pltpu.VMEM((8, 128), jnp.int32),
            pltpu.SMEM((8, 128), jnp.int32),
            dma((6,)),
            dma((n,)), dma((2, n)), dma((n,)), dma((2, n)),
            dma((2, 2, half * SUBS)), dma((2, 2, half * SUBS)),
            dma((2, 2, half * SUBS)), dma((2, 2, half * SUBS)),
            dma((3,)), dma((3,)),
            dma((n,)), dma((n,)),
            dma((2, n - 1)), dma((2, n - 1)),
            dma((n,)), dma((n,)),
        ],
        compiler_params=pltpu.CompilerParams(
            collective_id=0, has_side_effects=True, vmem_limit_bytes=57 * 1024 * 1024
        ),
    )(q_latent, q_rope, cache_latent, cache_rope, page_table, lengths)
    return out[None]


def solution(mesh):
    n = mesh.shape["head"]
    assert mesh.shape["seq"] == 2 * n and n % 2 == 0
    placed = (
        P(("grp", "seq"), "head", None),
        P(("grp", "seq"), "head", None),
        P(("grp", "seq", "head"), None, None),
        P(("grp", "seq", "head"), None, None),
        P(("grp", "seq"), None),
        P(("grp", "seq")),
    )
    return jax.shard_map(
        functools.partial(on_device, n),
        mesh=mesh,
        in_specs=placed,
        out_specs=P(("grp", "seq"), "head", None),
        check_vma=False,
    )
```

```python
import functools

import jax
import jax.numpy as jnp
from jax import lax
from jax.experimental import pallas as pl
from jax.experimental.pallas import tpu as pltpu
from jax.sharding import PartitionSpec as P

softmax_scale = 0.13528
floor_score = -1e30
MESH = pl.DeviceIdType.MESH
MOST = 4
STAT = 128
SUBS = 4
bf16, f32 = jnp.bfloat16, jnp.float32


def kernel(
    n, heads, lat_w, rope_w, page, slots,
    ql_hbm, qr_hbm, lat_hbm, rope_hbm, pt_hbm, len_ref,
    out_ref,
    lat, rope, QB, TB, SB, RB, LM, LT, LS, RR, MS, M2, FB, qown, town, qrv, ptv, tvm, tsm,
    loc, a_send, a_recv, t_send, t_recv, g_send, g_recv, d_send, d_recv, o_send, o_recv,
    p_send, p_recv, r_send, r_recv, f_send, f_recv,
):
    half = n // 2
    per = n // SUBS
    lanes = lat_w // 128
    sq = lax.axis_index("seq")
    x = lax.axis_index("head")
    y = sq // 2
    c = sq % 2
    a = x * (1 - c) + y * c
    b = y * (1 - c) + x * c

    def at(xx, yy, cc):
        return {"seq": 2 * yy + cc, "head": xx}

    sib = at(x, y, 1 - c)

    def rcopy(src, dst, ss, rs, dev):
        return pltpu.make_async_remote_copy(
            src_ref=src, dst_ref=dst, send_sem=ss, recv_sem=rs, device_id=dev, device_id_type=MESH
        )

    sends = []

    def send(src, dst, ss, rs, dev):
        cp = rcopy(src, dst, ss, rs, dev)
        cp.start()
        sends.append(cp)

    bar = pltpu.get_barrier_semaphore()
    far = sorted(range(1, n), key=lambda k: -min(k, n - k))
    partners = [at((x + k) % n, y, 1 - c) for k in far]
    partners += [at(x, (y + k) % n, 1 - c) for k in far]
    partners += [sib]
    ring = [at(x, (y + k) % n, 1) for k in far]
    ring += [at((x + 1) % n, y, 1), at((x + n - 1) % n, y, 1)]
    for dev in partners:
        pl.semaphore_signal(bar, inc=1, device_id=dev, device_id_type=MESH)

    @pl.when(c == 1)
    def _():
        for dev in ring:
            pl.semaphore_signal(bar, inc=1, device_id=dev, device_id_type=MESH)

    cq = pltpu.make_async_copy(ql_hbm.at[0], qown.at[:, pl.ds(0, lat_w)], loc.at[0])
    cs = pltpu.make_async_copy(qr_hbm.at[0], qrv, loc.at[1])
    ct = pltpu.make_async_copy(pt_hbm, ptv, loc.at[2])
    cl = pltpu.make_async_copy(lat_hbm, lat, loc.at[3])
    cr = pltpu.make_async_copy(rope_hbm, rope, loc.at[4])
    ct.start()
    cs.start()
    cq.start()
    cl.start()
    cr.start()

    ct.wait()
    rows_t = []
    lane1 = lax.broadcasted_iota(jnp.int32, (1, 128), 1)
    entries = ptv.shape[1] // 128
    for r in range(entries):
        v = ptv[:, r * 128 : (r + 1) * 128]
        live = jnp.clip(len_ref[0] - (lane1 + r * 128) * page, 0, page)
        rows_t.append(jnp.where(v >= 0, v * 256 + live, -1))
    rows_t.append(jnp.full((8 - entries, 128), -1, jnp.int32))
    town[...] = jnp.concatenate(rows_t, axis=0)
    cs.wait()
    qown[:, pl.ds(lat_w, STAT)] = jnp.concatenate(
        [qrv[...], jnp.zeros((heads, STAT - rope_w), bf16)], axis=1
    )
    cq.wait()

    pl.semaphore_wait(bar, len(partners) + len(ring) * c)

    for k in far:
        dev = at((x + k * (1 - c)) % n, (y + k * c) % n, 1)
        send(qown, QB.at[c, b, a], a_send.at[k], a_recv.at[c, k], dev)
    for k in far:
        send(town, TB.at[c, y], t_send.at[k], t_recv.at[c, k], at(x, (y + k) % n, 1))

    def part_of(par, idx, p):
        return QB.at[par, idx, pl.ds(p * per, per)]

    order = (
        tuple(range(SUBS)),
        tuple(range(SUBS // 2, SUBS)) + tuple(range(SUBS // 2)),
    )
    mid = (y, x)

    def origin(par, d, k):
        return (mid[par] + n - k) % n if d == 0 else (mid[par] + k) % n

    def subs_at(k):
        return SUBS // 2 if k == half else SUBS

    def build_table():
        first = (sq * n + x) * slots * 256
        codes = TB[...].reshape(n * 16, 128)
        ok = (codes >= first) & (codes < first + slots * 256)
        key = jnp.where(ok, codes - first, -1).T
        keys = [key] + [pltpu.roll(key, 128 - r, 1) for r in range(1, entries)]
        row = lax.broadcasted_iota(jnp.int32, (8, 128), 0)
        res = jnp.full((8, 128), -1, jnp.int32)
        for j in range(MOST):
            m = functools.reduce(jnp.maximum, keys)
            size = m.shape[0]
            while size > 8:
                size //= 2
                m = jnp.maximum(m[:size], m[size:])
            for r in (4, 2, 1):
                m = jnp.maximum(m, pltpu.roll(m, r, 0))
            res = jnp.where(row == j, m, res)
            full = jnp.concatenate([m] * (n * 2), axis=0)
            keys = [jnp.where(v == full, -1, v) for v in keys]
        tvm[...] = res
        cp = pltpu.make_async_copy(tvm, tsm, loc.at[5])
        cp.start()
        return cp

    def stats(top, total):
        hi = total.astype(bf16)
        lo = (total - hi.astype(f32)).astype(bf16)
        lane = lax.broadcasted_iota(jnp.int32, top.shape, 1)
        st = jnp.where(lane == 0, top, jnp.where(lane == 1, hi.astype(f32), lo.astype(f32)))
        return st.astype(bf16)

    def compute(par, yy, own):
        q = (QB[0, yy] if par == 0 else QB[1, :, yy]).reshape(n * heads, -1)
        ql, qr = q[:, :lat_w], q[:, lat_w : lat_w + rope_w]
        pages, ropes, counts = [], [], []
        for j in range(MOST):
            code = tsm[j, 8 * (par * n + yy)]
            slot = jnp.maximum(code, 0) // 256
            counts.append(jnp.where(code < 0, 0, code % 256))
            pages.append(lat[slot])
            ropes.append(rope[slot])
        keys = jnp.concatenate(pages, axis=0)
        sc = lax.dot_general(ql, keys, (((1,), (1,)), ((), ())), preferred_element_type=f32)
        sc = sc + jnp.dot(qr, jnp.concatenate(ropes, axis=1), preferred_element_type=f32)
        lane = lax.broadcasted_iota(jnp.int32, (n * heads, page), 1)
        live = [lane < v for v in counts]
        parts = [
            jnp.where(live[j], sc[:, j * page : (j + 1) * page] * softmax_scale, floor_score)
            for j in range(MOST)
        ]
        top = functools.reduce(jnp.maximum, parts)
        top = jnp.max(top, axis=1, keepdims=True).astype(bf16).astype(f32)
        ws = [jnp.where(o, jnp.exp(s - top), 0.0) for o, s in zip(live, parts)]
        total = jnp.sum(ws[0] + ws[1] + ws[2] + ws[3], axis=1, keepdims=True)
        w = jnp.concatenate([v.astype(bf16) for v in ws], axis=1)
        mixed = jnp.dot(w, keys, preferred_element_type=f32)
        top = jnp.broadcast_to(top, (n * heads, STAT))
        total = jnp.broadcast_to(total, (n * heads, STAT))
        shape = (n, heads, -1)

        if own:
            for ref, v in ((LM, mixed), (LT, top), (LS, total)):
                if par == 0:
                    ref[0, yy] = v.reshape(shape)
                else:
                    ref[1, :, yy] = v.reshape(shape)
        else:
            full = jnp.concatenate([mixed.astype(bf16), stats(top, total)], axis=1)
            SB[par, yy] = full.reshape(shape)
            dst = RB.at[0, yy] if par == 0 else RB.at[1, :, yy]
            i = par * n + yy
            rcopy(SB.at[par, yy], dst, p_send.at[i], p_recv.at[i], sib).start()

    rows = per * heads
    er = lax.broadcasted_iota(jnp.int32, (STAT, 2 * STAT), 0)
    ec = lax.broadcasted_iota(jnp.int32, (STAT, 2 * STAT), 1)
    spread = jnp.where(
        ((er == 0) & (ec < STAT)) | ((er > 0) & (er < 3) & (ec >= STAT)), 1.0, 0.0
    ).astype(bf16)

    def opened(v):
        s = jnp.dot(v[:, lat_w:], spread, preferred_element_type=f32)
        tiles = [v[:, j * 128 : (j + 1) * 128].astype(f32) for j in range(lanes)]
        return tiles, s[:, :STAT], s[:, STAT:]

    def merge(states):
        top = functools.reduce(jnp.maximum, [s[1] for s in states])
        fac = [jnp.exp(s[1] - top) for s in states]
        total = sum(f * s[2] for f, s in zip(fac, states))
        tiles = [sum(f * s[0][j] for f, s in zip(fac, states)) for j in range(lanes)]
        return tiles, top, total

    def packed(state):
        tiles, top, total = state
        return jnp.concatenate([t.astype(bf16) for t in tiles] + [stats(top, total)], axis=1)

    def ps(p):
        return pl.ds(p * per, per)

    def both(par, idx, p):
        v = LM[par, idx, ps(p)].reshape(rows, lat_w)
        tiles = [v[:, j * 128 : (j + 1) * 128] for j in range(lanes)]
        top = LT[par, idx, ps(p)].reshape(rows, STAT)
        total = LS[par, idx, ps(p)].reshape(rows, STAT)
        return [(tiles, top, total), opened(RB[par, idx, ps(p)].reshape(rows, -1))]

    def goal(par, d, k):
        return (mid[par] + k) % n if d == 0 else (mid[par] + n - k) % n

    def halves(d):
        lo, hi = tuple(range(SUBS // 2)), tuple(range(SUBS // 2, SUBS))
        return (hi, lo) if d == 0 else (lo, hi)

    def owned(values):
        tiles, top, total = merge(values)
        out_ref[...] = jnp.concatenate([(t / total).astype(bf16) for t in tiles], axis=1)

    @pl.when(c == 1)
    def _():
        out = []

        def put(src, dst, ss, rs, dev):
            cp = rcopy(src, dst, ss, rs, dev)
            cp.start()
            out.append(cp)

        neighbour = (
            (at(x, (y + 1) % n, 1), at(x, (y + n - 1) % n, 1)),
            (at((x + 1) % n, y, 1), at((x + n - 1) % n, y, 1)),
        )
        QB[1, x, y] = qown[...]
        TB[1, y] = town[...]
        for par in (1, 0):
            for k in far + ([0] if par == 0 else []):
                src = (x + n - k) % n if par == 0 else (y + n - k) % n
                part = QB.at[par, mid[par], src]
                rcopy(part, part, a_send.at[k], a_recv.at[par, k], sib).wait_recv()
            for j in range(SUBS):
                for d in range(2):
                    p = order[d][j]
                    part = part_of(par, mid[par], p)
                    put(part, part, g_send.at[par, d, p], g_recv.at[par, d, p], neighbour[par][d])
            part = QB.at[par, mid[par]]
            put(part, part, o_send.at[par], o_recv.at[par], sib)
        def ring_sub(k, j):
            for par in (1, 0):
                for d in range(2):
                    p = order[d][j]
                    i = (k - 1) * SUBS + p
                    part = part_of(par, origin(par, d, k), p)
                    rcopy(part, part, g_send.at[par, d, i], g_recv.at[par, d, i], sib).wait_recv()
                    if k < half - 1 or (k == half - 1 and j < SUBS // 2):
                        i2 = i + SUBS
                        ss, rs = g_send.at[par, d, i2], g_recv.at[par, d, i2]
                        put(part, part, ss, rs, neighbour[par][d])
                    put(part, part, d_send.at[par, d, i], d_recv.at[par, d, i], sib)

        def ring_all(k):
            for j in range(subs_at(k)):
                ring_sub(k, j)

        ring_all(1)
        for par in (1, 0):
            for k in far + ([0] if par == 0 else []):
                part = TB.at[par, (y + n - k) % n]
                rcopy(part, part, t_send.at[k], t_recv.at[par, k], sib).wait_recv()
        put(TB, TB, o_send.at[2], o_recv.at[2], sib)
        built = build_table()
        cl.wait()
        cr.wait()
        ring_all(2)
        built.wait()
        compute(0, y, True)
        ring_all(3)
        compute(0, (y + 1) % n, True)
        ring_all(half)

        def evens(i, carry):
            compute(0, (y + n + (i + 3) // 2 * (1 - 2 * ((i + 1) % 2))) % n, True)
            return carry

        lax.fori_loop(0, n - 2, evens, 0)

        def odds(first, last):
            def body(i, carry):
                compute(1, i, True)
                return carry

            lax.fori_loop(first, last, body, 0)

        def index(k, p):
            return p % (SUBS // 2) if k == 1 else SUBS // 2 + (k - 2) * SUBS + p

        def sibling_states(par):
            for i in range(n):
                part = RB.at[par, i]
                rcopy(
                    part, part, p_send.at[par * n + i], p_recv.at[par * n + i], sib
                ).wait_recv()

        def ring_send(par, d, k, p, states):
            i = index(k, p)
            MS[par, d, i] = packed(merge(states)).reshape(per, heads, -1)
            ss, rs = r_send.at[par, d, i], r_recv.at[par, d, i]
            put(MS.at[par, d, i], RR.at[par, d, i], ss, rs, neighbour[par][d])

        def ring_recv(par, d, k, p):
            i = index(k, p)
            part = RR.at[par, d, i]
            rcopy(part, part, r_send.at[par, d, i], r_recv.at[par, d, i], sib).wait_recv()
            return [opened(RR[par, d, i].reshape(rows, -1))]

        def open_ring(par):
            for p in range(SUBS // 2):
                for d in range(2):
                    q = halves(d)[1][p]
                    ring_send(par, d, 1, q, both(par, goal(par, d, half), q))
            for p in range(SUBS // 2):
                for d in range(2):
                    q = halves(d)[0][p]
                    ring_send(par, d, 2, q, both(par, goal(par, d, half - 1), q))

        def ring_step(pars, ks, js):
            for j in js:
                for par, k in zip(pars, ks):
                    for d in range(2):
                        p = (halves(d)[0] + halves(d)[1])[j]
                        own = both(par, goal(par, d, half + 1 - k), p)
                        ring_send(par, d, k, p, own + ring_recv(par, d, k - 1, p))

        def close_ring(par):
            for p in range(SUBS):
                own = both(par, mid[par], p)
                state = own + ring_recv(par, 0, half, p) + ring_recv(par, 1, half, p)
                M2[par, ps(p)] = packed(merge(state)).reshape(per, heads, -1)
            for k in far:
                if par == 0:
                    o, dev = (x + k) % n, at((x + k) % n, y, 0)
                else:
                    o, dev = (y + k) % n, at(x, (y + k) % n, 1)
                put(M2.at[par, o], FB.at[k], f_send.at[par, k], f_recv.at[k], dev)
            if par == 0:
                put(M2.at[0, x], FB.at[0], f_send.at[0, 0], f_recv.at[0], sib)

        late = range(SUBS // 2, SUBS)
        every = range(SUBS)
        sibling_states(0)
        open_ring(0)
        odds(0, 5)
        ring_step((0,), (2,), late)
        odds(5, n)
        sibling_states(1)
        open_ring(1)
        ring_step((0,), (3,), every)
        ring_step((1,), (2,), late)
        ring_step((0, 1), (4, 3), every)
        close_ring(0)
        ring_step((1,), (4,), every)
        close_ring(1)
        states = [opened(M2[1, y])]
        for k in far:
            rcopy(FB.at[k], FB.at[k], f_send.at[1, k], f_recv.at[k], sib).wait_recv()
            states.append(opened(FB[k]))
        owned(states)
        for cp in out:
            cp.wait_send()

    @pl.when(c == 0)
    def _():
        put_a = rcopy(qown, QB.at[0, y, x], a_send.at[0], a_recv.at[0, 0], sib)
        put_t = rcopy(town, TB.at[0, y], t_send.at[0], t_recv.at[0, 0], sib)
        put_a.start()
        put_t.start()

        def arrived(par, k):
            if k == 0:
                part = QB.at[par, mid[par]]
                rcopy(part, part, o_send.at[par], o_recv.at[par], sib).wait_recv()
                return
            for j in range(subs_at(k)):
                for d in range(2):
                    p = order[d][j]
                    i = (k - 1) * SUBS + p
                    part = part_of(par, origin(par, d, k), p)
                    rcopy(part, part, d_send.at[par, d, i], d_recv.at[par, d, i], sib).wait_recv()

        rcopy(TB, TB, o_send.at[2], o_recv.at[2], sib).wait_recv()
        built = build_table()
        cl.wait()
        cr.wait()
        arrived(0, 0)
        built.wait()
        compute(0, y, False)
        for k in range(1, half + 1):
            arrived(0, k)
            compute(0, (y + n - k) % n, False)
            if k < half:
                compute(0, (y + k) % n, False)
        for k in range(half + 1):
            arrived(1, k)

        def body(i, carry):
            compute(1, i, False)
            return carry

        lax.fori_loop(0, n, body, 0)
        states = []
        for k in far + [0]:
            rcopy(FB.at[k], FB.at[k], f_send.at[0, k], f_recv.at[k], sib).wait_recv()
            states.append(opened(FB[k]))
        owned(states)
        for i in range(2 * n):
            part = SB.at[i // n, i % n]
            rcopy(part, part, p_send.at[i], p_recv.at[i], sib).wait_send()
        put_a.wait_send()
        put_t.wait_send()

    for cp in sends:
        cp.wait_send()


def on_device(n, q_latent, q_rope, cache_latent, cache_rope, page_table, lengths):
    heads, lat_w = q_latent.shape[1:]
    rope_w = q_rope.shape[2]
    slots, page, _ = cache_latent.shape
    width = lat_w + STAT
    half, per = n // 2, n // SUBS
    messages = (half - 1) * SUBS + SUBS // 2
    any_spec = pl.BlockSpec(memory_space=pl.ANY)
    dma = pltpu.SemaphoreType.DMA
    out = pl.pallas_call(
        functools.partial(kernel, n, heads, lat_w, rope_w, page, slots),
        out_shape=jax.ShapeDtypeStruct((heads, lat_w), bf16),
        in_specs=[any_spec] * 5 + [pl.BlockSpec(memory_space=pltpu.SMEM)],
        out_specs=pl.BlockSpec(memory_space=pltpu.VMEM),
        scratch_shapes=[
            pltpu.VMEM(cache_latent.shape, bf16),
            pltpu.VMEM(cache_rope.shape, bf16),
            pltpu.VMEM((2, n, n, heads, width), bf16),
            pltpu.VMEM((2, n, 8, 128), jnp.int32),
            pltpu.VMEM((2, n, n, heads, width), bf16),
            pltpu.VMEM((2, n, n, heads, width), bf16),
            pltpu.VMEM((2, n, n, heads, lat_w), f32),
            pltpu.VMEM((2, n, n, heads, STAT), f32),
            pltpu.VMEM((2, n, n, heads, STAT), f32),
            pltpu.VMEM((2, 2, messages, per, heads, width), bf16),
            pltpu.VMEM((2, 2, messages, per, heads, width), bf16),
            pltpu.VMEM((2, n, heads, width), bf16),
            pltpu.VMEM((n, heads, width), bf16),
            pltpu.VMEM((heads, width), bf16),
            pltpu.VMEM((8, 128), jnp.int32),
            pltpu.VMEM((heads, rope_w), bf16),
            pltpu.VMEM(page_table.shape, jnp.int32),
            pltpu.VMEM((8, 128), jnp.int32),
            pltpu.SMEM((8, 128), jnp.int32),
            dma((6,)),
            dma((n,)), dma((2, n)), dma((n,)), dma((2, n)),
            dma((2, 2, half * SUBS)), dma((2, 2, half * SUBS)),
            dma((2, 2, half * SUBS)), dma((2, 2, half * SUBS)),
            dma((3,)), dma((3,)),
            dma((2 * n,)), dma((2 * n,)),
            dma((2, 2, messages)), dma((2, 2, messages)),
            dma((2, n)), dma((n,)),
        ],
        compiler_params=pltpu.CompilerParams(
            collective_id=0, has_side_effects=True, vmem_limit_bytes=57 * 1024 * 1024
        ),
    )(q_latent, q_rope, cache_latent, cache_rope, page_table, lengths)
    return out[None]


def solution(mesh):
    n = mesh.shape["head"]
    assert n == 8 and mesh.shape["seq"] == 2 * n
    placed = (
        P(("grp", "seq"), "head", None),
        P(("grp", "seq"), "head", None),
        P(("grp", "seq", "head"), None, None),
        P(("grp", "seq", "head"), None, None),
        P(("grp", "seq"), None),
        P(("grp", "seq")),
    )
    return jax.shard_map(
        functools.partial(on_device, n),
        mesh=mesh,
        in_specs=placed,
        out_specs=P(("grp", "seq"), "head", None),
        check_vma=False,
    )
```

```python
import functools

import jax
import jax.numpy as jnp
from jax import lax
from jax.experimental import pallas as pl
from jax.experimental.pallas import tpu as pltpu
from jax.sharding import PartitionSpec as P

softmax_scale = 0.13528
floor_score = -1e30
MESH = pl.DeviceIdType.MESH
MOST = 4
STAT = 128
SUBS = 4
bf16, f32 = jnp.bfloat16, jnp.float32


def kernel(
    n, heads, lat_w, rope_w, page, slots,
    ql_hbm, qr_hbm, lat_hbm, rope_hbm, pt_hbm, len_ref,
    out_ref,
    lat, rope, QB, TB, SB, RB, LM, LT, LS, RR, MS, M2, FB, qown, town, qrv, ptv, tvm, tsm,
    loc, a_send, a_recv, t_send, t_recv, g_send, g_recv, d_send, d_recv, o_send, o_recv,
    p_send, p_recv, r_send, r_recv, f_send, f_recv,
):
    half = n // 2
    per = n // SUBS
    lanes = lat_w // 128
    sq = lax.axis_index("seq")
    x = lax.axis_index("head")
    y = sq // 2
    c = sq % 2
    a = x * (1 - c) + y * c
    b = y * (1 - c) + x * c

    def at(xx, yy, cc):
        return {"seq": 2 * yy + cc, "head": xx}

    def dev_a(i):
        return at(i * (1 - c) + x * c, y * (1 - c) + i * c, c)

    def dev_b(i):
        return at(x * (1 - c) + i * c, i * (1 - c) + y * c, c)

    sib = at(x, y, 1 - c)

    def rcopy(src, dst, ss, rs, dev):
        return pltpu.make_async_remote_copy(
            src_ref=src, dst_ref=dst, send_sem=ss, recv_sem=rs, device_id=dev, device_id_type=MESH
        )

    sends = []

    def send(src, dst, ss, rs, dev):
        cp = rcopy(src, dst, ss, rs, dev)
        cp.start()
        sends.append(cp)

    bar = pltpu.get_barrier_semaphore()
    far = sorted(range(1, n), key=lambda k: -min(k, n - k))
    partners = [at((x + k) % n, y, 1 - c) for k in far]
    partners += [at(x, (y + k) % n, 1 - c) for k in far]
    partners += [dev_a((a + k) % n) for k in far]
    partners += [dev_b((b + 1) % n), dev_b((b + n - 1) % n), sib]
    for dev in partners:
        pl.semaphore_signal(bar, inc=1, device_id=dev, device_id_type=MESH)

    cq = pltpu.make_async_copy(ql_hbm.at[0], qown.at[:, pl.ds(0, lat_w)], loc.at[0])
    cs = pltpu.make_async_copy(qr_hbm.at[0], qrv, loc.at[1])
    ct = pltpu.make_async_copy(pt_hbm, ptv, loc.at[2])
    cl = pltpu.make_async_copy(lat_hbm, lat, loc.at[3])
    cr = pltpu.make_async_copy(rope_hbm, rope, loc.at[4])
    ct.start()
    cs.start()
    cq.start()
    cl.start()
    cr.start()

    ct.wait()
    rows_t = []
    lane1 = lax.broadcasted_iota(jnp.int32, (1, 128), 1)
    entries = ptv.shape[1] // 128
    for r in range(entries):
        v = ptv[:, r * 128 : (r + 1) * 128]
        live = jnp.clip(len_ref[0] - (lane1 + r * 128) * page, 0, page)
        rows_t.append(jnp.where(v >= 0, v * 256 + live, -1))
    rows_t.append(jnp.full((8 - entries, 128), -1, jnp.int32))
    town[...] = jnp.concatenate(rows_t, axis=0)
    cs.wait()
    qown[:, pl.ds(lat_w, STAT)] = jnp.concatenate(
        [qrv[...], jnp.zeros((heads, STAT - rope_w), bf16)], axis=1
    )
    cq.wait()

    pl.semaphore_wait(bar, len(partners))

    for k in far:
        dev = at((x + k * (1 - c)) % n, (y + k * c) % n, 1)
        send(qown, QB.at[c, b, a], a_send.at[k], a_recv.at[c, k], dev)
    for k in far:
        send(town, TB.at[c, y], t_send.at[k], t_recv.at[c, k], at(x, (y + k) % n, 1))

    def part_of(par, idx, p):
        return QB.at[par, idx, pl.ds(p * per, per)]

    order = (
        tuple(range(SUBS)),
        tuple(range(SUBS // 2, SUBS)) + tuple(range(SUBS // 2)),
    )
    mid = (y, x)

    def origin(par, d, k):
        return (mid[par] + n - k) % n if d == 0 else (mid[par] + k) % n

    def subs_at(k):
        return SUBS // 2 if k == half else SUBS

    def build_table():
        first = (sq * n + x) * slots * 256
        codes = TB[...].reshape(n * 16, 128)
        ok = (codes >= first) & (codes < first + slots * 256)
        key = jnp.where(ok, codes - first, -1).T
        keys = [key] + [pltpu.roll(key, 128 - r, 1) for r in range(1, entries)]
        row = lax.broadcasted_iota(jnp.int32, (8, 128), 0)
        res = jnp.full((8, 128), -1, jnp.int32)
        for j in range(MOST):
            m = functools.reduce(jnp.maximum, keys)
            size = m.shape[0]
            while size > 8:
                size //= 2
                m = jnp.maximum(m[:size], m[size:])
            for r in (4, 2, 1):
                m = jnp.maximum(m, pltpu.roll(m, r, 0))
            res = jnp.where(row == j, m, res)
            full = jnp.concatenate([m] * (n * 2), axis=0)
            keys = [jnp.where(v == full, -1, v) for v in keys]
        tvm[...] = res
        cp = pltpu.make_async_copy(tvm, tsm, loc.at[5])
        cp.start()
        return cp

    def stats(top, total):
        hi = total.astype(bf16)
        lo = (total - hi.astype(f32)).astype(bf16)
        lane = lax.broadcasted_iota(jnp.int32, top.shape, 1)
        st = jnp.where(lane == 0, top, jnp.where(lane == 1, hi.astype(f32), lo.astype(f32)))
        return st.astype(bf16)

    def compute(par, yy, own):
        q = (QB[0, yy] if par == 0 else QB[1, :, yy]).reshape(n * heads, -1)
        ql, qr = q[:, :lat_w], q[:, lat_w : lat_w + rope_w]
        pages, ropes, counts = [], [], []
        for j in range(MOST):
            code = tsm[j, 8 * (par * n + yy)]
            slot = jnp.maximum(code, 0) // 256
            counts.append(jnp.where(code < 0, 0, code % 256))
            pages.append(lat[slot])
            ropes.append(rope[slot])
        keys = jnp.concatenate(pages, axis=0)
        sc = lax.dot_general(ql, keys, (((1,), (1,)), ((), ())), preferred_element_type=f32)
        sc = sc + jnp.dot(qr, jnp.concatenate(ropes, axis=1), preferred_element_type=f32)
        lane = lax.broadcasted_iota(jnp.int32, (n * heads, page), 1)
        live = [lane < v for v in counts]
        parts = [
            jnp.where(live[j], sc[:, j * page : (j + 1) * page] * softmax_scale, floor_score)
            for j in range(MOST)
        ]
        top = functools.reduce(jnp.maximum, parts)
        top = jnp.max(top, axis=1, keepdims=True).astype(bf16).astype(f32)
        ws = [jnp.where(o, jnp.exp(s - top), 0.0) for o, s in zip(live, parts)]
        total = jnp.sum(ws[0] + ws[1] + ws[2] + ws[3], axis=1, keepdims=True)
        w = jnp.concatenate([v.astype(bf16) for v in ws], axis=1)
        mixed = jnp.dot(w, keys, preferred_element_type=f32)
        top = jnp.broadcast_to(top, (n * heads, STAT))
        total = jnp.broadcast_to(total, (n * heads, STAT))
        shape = (n, heads, -1)

        if own and par == 0:
            LM[yy] = mixed.reshape(shape)
            LT[yy] = top.reshape(shape)
            LS[yy] = total.reshape(shape)
        elif own:
            LM[:, yy] = mixed.reshape(shape)
            LT[:, yy] = top.reshape(shape)
            LS[:, yy] = total.reshape(shape)
        else:
            full = jnp.concatenate([mixed.astype(bf16), stats(top, total)], axis=1)
            SB[yy] = full.reshape(shape)
            dst = RB.at[yy] if par == 0 else RB.at[:, yy]
            rcopy(SB.at[yy], dst, p_send.at[yy], p_recv.at[yy], sib).start()

    rows = per * heads
    er = lax.broadcasted_iota(jnp.int32, (STAT, 2 * STAT), 0)
    ec = lax.broadcasted_iota(jnp.int32, (STAT, 2 * STAT), 1)
    spread = jnp.where(
        ((er == 0) & (ec < STAT)) | ((er > 0) & (er < 3) & (ec >= STAT)), 1.0, 0.0
    ).astype(bf16)

    def opened(v):
        s = jnp.dot(v[:, lat_w:], spread, preferred_element_type=f32)
        tiles = [v[:, j * 128 : (j + 1) * 128].astype(f32) for j in range(lanes)]
        return tiles, s[:, :STAT], s[:, STAT:]

    def merge(states):
        top = functools.reduce(jnp.maximum, [s[1] for s in states])
        fac = [jnp.exp(s[1] - top) for s in states]
        total = sum(f * s[2] for f, s in zip(fac, states))
        tiles = [sum(f * s[0][j] for f, s in zip(fac, states)) for j in range(lanes)]
        return tiles, top, total

    def packed(state):
        tiles, top, total = state
        return jnp.concatenate([t.astype(bf16) for t in tiles] + [stats(top, total)], axis=1)

    def ps(p):
        return pl.ds(p * per, per)

    def both(idx, p):
        v = LM[idx, ps(p)].reshape(rows, lat_w)
        tiles = [v[:, j * 128 : (j + 1) * 128] for j in range(lanes)]
        top = LT[idx, ps(p)].reshape(rows, STAT)
        total = LS[idx, ps(p)].reshape(rows, STAT)
        return [(tiles, top, total), opened(RB[idx, ps(p)].reshape(rows, -1))]

    def goal(d, k):
        return (b + k) % n if d == 0 else (b + n - k) % n

    nxt = (dev_b((b + 1) % n), dev_b((b + n - 1) % n))
    halves = (
        (tuple(range(SUBS // 2, SUBS)), tuple(range(SUBS // 2))),
        (tuple(range(SUBS // 2)), tuple(range(SUBS // 2, SUBS))),
    )

    def reduce():
        out = []

        def put(src, dst, ss, rs, dev):
            cp = rcopy(src, dst, ss, rs, dev)
            cp.start()
            out.append(cp)

        def index(k, p):
            return p % (SUBS // 2) if k == 1 else SUBS // 2 + (k - 2) * SUBS + p

        def wait(d, k, p):
            i = index(k, p)
            part = RR.at[d, i]
            rcopy(part, part, r_send.at[d, i], r_recv.at[d, i], sib).wait_recv()

        def got(d, k, p):
            return [opened(RR[d, index(k, p)].reshape(rows, -1))]

        def step(k, subs, arrives):
            states = [both(goal(d, half + 1 - k), subs[d]) for d in range(2)]
            if arrives:
                for d in range(2):
                    wait(d, k - 1, subs[d])
                states = [states[d] + got(d, k - 1, subs[d]) for d in range(2)]
            full = [packed(merge(v)) for v in states]
            for d in range(2):
                MS[d, index(k, subs[d])] = full[d].reshape(per, heads, -1)
            for d in range(2):
                i = index(k, subs[d])
                put(MS.at[d, i], RR.at[d, i], r_send.at[d, i], r_recv.at[d, i], nxt[d])

        for i in range(n):
            rcopy(RB.at[i], RB.at[i], p_send.at[i], p_recv.at[i], sib).wait_recv()
        first, late = [tuple(zip(halves[0][h], halves[1][h])) for h in range(2)]
        for subs in late:
            step(1, subs, False)
        for subs in first:
            step(2, subs, False)
        for subs in late:
            step(2, subs, True)
        for k in range(3, half + 1):
            for subs in first + late:
                step(k, subs, True)
        for j in range(0, SUBS, 2):
            states = [both(b, p) for p in (j, j + 1)]
            for p in (j, j + 1):
                for d in range(2):
                    wait(d, half, p)
            full = [
                packed(merge(v + got(0, half, p) + got(1, half, p)))
                for v, p in zip(states, (j, j + 1))
            ]
            for v, p in zip(full, (j, j + 1)):
                M2[ps(p)] = v.reshape(per, heads, -1)
        for k in far:
            o = (a + k) % n
            put(M2.at[o], FB.at[k], f_send.at[k], f_recv.at[k], dev_a(o))
        for k in far:
            rcopy(FB.at[k], FB.at[k], f_send.at[k], f_recv.at[k], sib).wait_recv()
        tiles, top, total = merge([opened(M2[a])] + [opened(FB[k]) for k in far])
        out_ref[...] = jnp.concatenate([(t / total).astype(bf16) for t in tiles], axis=1)
        for i in range(n):
            rcopy(SB.at[i], SB.at[i], p_send.at[i], p_recv.at[i], sib).wait_send()
        for cp in out:
            cp.wait_send()

    @pl.when(c == 1)
    def _():
        out = []

        def put(src, dst, ss, rs, dev):
            cp = rcopy(src, dst, ss, rs, dev)
            cp.start()
            out.append(cp)

        neighbour = (
            (at(x, (y + 1) % n, 1), at(x, (y + n - 1) % n, 1)),
            (at((x + 1) % n, y, 1), at((x + n - 1) % n, y, 1)),
        )
        QB[1, x, y] = qown[...]
        TB[1, y] = town[...]
        for par in (1, 0):
            for k in far + ([0] if par == 0 else []):
                src = (x + n - k) % n if par == 0 else (y + n - k) % n
                part = QB.at[par, mid[par], src]
                rcopy(part, part, a_send.at[k], a_recv.at[par, k], sib).wait_recv()
            for j in range(SUBS):
                for d in range(2):
                    p = order[d][j]
                    part = part_of(par, mid[par], p)
                    put(part, part, g_send.at[par, d, p], g_recv.at[par, d, p], neighbour[par][d])
            part = QB.at[par, mid[par]]
            put(part, part, o_send.at[par], o_recv.at[par], sib)
        def ring_sub(k, j):
            for par in (1, 0):
                for d in range(2):
                    p = order[d][j]
                    i = (k - 1) * SUBS + p
                    part = part_of(par, origin(par, d, k), p)
                    rcopy(part, part, g_send.at[par, d, i], g_recv.at[par, d, i], sib).wait_recv()
                    if k < half - 1 or (k == half - 1 and j < SUBS // 2):
                        i2 = i + SUBS
                        ss, rs = g_send.at[par, d, i2], g_recv.at[par, d, i2]
                        put(part, part, ss, rs, neighbour[par][d])
                    put(part, part, d_send.at[par, d, i], d_recv.at[par, d, i], sib)

        def ring_all(k):
            for j in range(subs_at(k)):
                ring_sub(k, j)

        ring_all(1)
        for par in (1, 0):
            for k in far + ([0] if par == 0 else []):
                part = TB.at[par, (y + n - k) % n]
                rcopy(part, part, t_send.at[k], t_recv.at[par, k], sib).wait_recv()
        put(TB, TB, o_send.at[2], o_recv.at[2], sib)
        built = build_table()
        cl.wait()
        cr.wait()
        ring_all(2)
        built.wait()
        compute(0, y, False)
        ring_all(3)
        compute(0, (y + 1) % n, False)
        ring_all(half)

        def evens(i, carry):
            compute(0, (y + n + (i + 3) // 2 * (1 - 2 * ((i + 1) % 2))) % n, False)
            return carry

        lax.fori_loop(0, n - 2, evens, 0)

        def odd(i, carry):
            compute(1, i, True)
            return carry

        lax.fori_loop(0, n, odd, 0)
        reduce()
        for cp in out:
            cp.wait_send()

    @pl.when(c == 0)
    def _():
        put_a = rcopy(qown, QB.at[0, y, x], a_send.at[0], a_recv.at[0, 0], sib)
        put_t = rcopy(town, TB.at[0, y], t_send.at[0], t_recv.at[0, 0], sib)
        put_a.start()
        put_t.start()

        def arrived(par, k):
            if k == 0:
                part = QB.at[par, mid[par]]
                rcopy(part, part, o_send.at[par], o_recv.at[par], sib).wait_recv()
                return
            for j in range(subs_at(k)):
                for d in range(2):
                    p = order[d][j]
                    i = (k - 1) * SUBS + p
                    part = part_of(par, origin(par, d, k), p)
                    rcopy(part, part, d_send.at[par, d, i], d_recv.at[par, d, i], sib).wait_recv()

        rcopy(TB, TB, o_send.at[2], o_recv.at[2], sib).wait_recv()
        built = build_table()
        cl.wait()
        cr.wait()
        arrived(0, 0)
        built.wait()
        compute(0, y, True)
        for k in range(1, half + 1):
            arrived(0, k)
            compute(0, (y + n - k) % n, True)
            if k < half:
                compute(0, (y + k) % n, True)
        for k in range(half + 1):
            arrived(1, k)

        def odd(i, carry):
            compute(1, i, False)
            return carry

        lax.fori_loop(0, n, odd, 0)
        reduce()
        put_a.wait_send()
        put_t.wait_send()

    for cp in sends:
        cp.wait_send()


def on_device(n, q_latent, q_rope, cache_latent, cache_rope, page_table, lengths):
    heads, lat_w = q_latent.shape[1:]
    rope_w = q_rope.shape[2]
    slots, page, _ = cache_latent.shape
    width = lat_w + STAT
    half, per = n // 2, n // SUBS
    messages = (half - 1) * SUBS + SUBS // 2
    any_spec = pl.BlockSpec(memory_space=pl.ANY)
    dma = pltpu.SemaphoreType.DMA
    out = pl.pallas_call(
        functools.partial(kernel, n, heads, lat_w, rope_w, page, slots),
        out_shape=jax.ShapeDtypeStruct((heads, lat_w), bf16),
        in_specs=[any_spec] * 5 + [pl.BlockSpec(memory_space=pltpu.SMEM)],
        out_specs=pl.BlockSpec(memory_space=pltpu.VMEM),
        scratch_shapes=[
            pltpu.VMEM(cache_latent.shape, bf16),
            pltpu.VMEM(cache_rope.shape, bf16),
            pltpu.VMEM((2, n, n, heads, width), bf16),
            pltpu.VMEM((2, n, 8, 128), jnp.int32),
            pltpu.VMEM((n, n, heads, width), bf16),
            pltpu.VMEM((n, n, heads, width), bf16),
            pltpu.VMEM((n, n, heads, lat_w), f32),
            pltpu.VMEM((n, n, heads, STAT), f32),
            pltpu.VMEM((n, n, heads, STAT), f32),
            pltpu.VMEM((2, messages, per, heads, width), bf16),
            pltpu.VMEM((2, messages, per, heads, width), bf16),
            pltpu.VMEM((n, heads, width), bf16),
            pltpu.VMEM((n, heads, width), bf16),
            pltpu.VMEM((heads, width), bf16),
            pltpu.VMEM((8, 128), jnp.int32),
            pltpu.VMEM((heads, rope_w), bf16),
            pltpu.VMEM(page_table.shape, jnp.int32),
            pltpu.VMEM((8, 128), jnp.int32),
            pltpu.SMEM((8, 128), jnp.int32),
            dma((6,)),
            dma((n,)), dma((2, n)), dma((n,)), dma((2, n)),
            dma((2, 2, half * SUBS)), dma((2, 2, half * SUBS)),
            dma((2, 2, half * SUBS)), dma((2, 2, half * SUBS)),
            dma((3,)), dma((3,)),
            dma((n,)), dma((n,)),
            dma((2, messages)), dma((2, messages)),
            dma((n,)), dma((n,)),
        ],
        compiler_params=pltpu.CompilerParams(
            collective_id=0, has_side_effects=True, vmem_limit_bytes=57 * 1024 * 1024
        ),
    )(q_latent, q_rope, cache_latent, cache_rope, page_table, lengths)
    return out[None]


def solution(mesh):
    n = mesh.shape["head"]
    assert n == 8 and mesh.shape["seq"] == 2 * n
    placed = (
        P(("grp", "seq"), "head", None),
        P(("grp", "seq"), "head", None),
        P(("grp", "seq", "head"), None, None),
        P(("grp", "seq", "head"), None, None),
        P(("grp", "seq"), None),
        P(("grp", "seq")),
    )
    return jax.shard_map(
        functools.partial(on_device, n),
        mesh=mesh,
        in_specs=placed,
        out_specs=P(("grp", "seq"), "head", None),
        check_vma=False,
    )
```

```python
import functools

import jax
import jax.numpy as jnp
from jax import lax
from jax.experimental import pallas as pl
from jax.experimental.pallas import tpu as pltpu
from jax.sharding import PartitionSpec as P

softmax_scale = 0.13528
floor_score = -1e30
MESH = pl.DeviceIdType.MESH
MOST = 4
STAT = 128
SUBS = 4
bf16, f32 = jnp.bfloat16, jnp.float32


def kernel(
    n, heads, lat_w, rope_w, page, slots,
    ql_hbm, qr_hbm, lat_hbm, rope_hbm, pt_hbm, len_ref,
    out_ref,
    lat, rope, QB, TB, SB, RB, LM, LT, LS, RR, MS, M2, FB, qown, town, qrv, ptv, tvm, tsm,
    loc, a_send, a_recv, t_send, t_recv, g_send, g_recv, d_send, d_recv, o_send, o_recv,
    p_send, p_recv, r_send, r_recv, f_send, f_recv,
):
    half = n // 2
    per = n // SUBS
    lanes = lat_w // 128
    sq = lax.axis_index("seq")
    x = lax.axis_index("head")
    y = sq // 2
    c = sq % 2
    a = x * (1 - c) + y * c
    b = y * (1 - c) + x * c

    def at(xx, yy, cc):
        return {"seq": 2 * yy + cc, "head": xx}

    def dev_a(i):
        return at(i * (1 - c) + x * c, y * (1 - c) + i * c, c)

    def dev_b(i):
        return at(x * (1 - c) + i * c, i * (1 - c) + y * c, c)

    sib = at(x, y, 1 - c)

    def rcopy(src, dst, ss, rs, dev):
        return pltpu.make_async_remote_copy(
            src_ref=src, dst_ref=dst, send_sem=ss, recv_sem=rs, device_id=dev, device_id_type=MESH
        )

    sends = []

    def send(src, dst, ss, rs, dev):
        cp = rcopy(src, dst, ss, rs, dev)
        cp.start()
        sends.append(cp)

    bar = pltpu.get_barrier_semaphore()
    far = sorted(range(1, n), key=lambda k: -min(k, n - k))
    partners = [at((x + k) % n, y, 1 - c) for k in far]
    partners += [at(x, (y + k) % n, 1 - c) for k in far]
    partners += [dev_a((a + k) % n) for k in far]
    partners += [dev_b((b + 1) % n), dev_b((b + n - 1) % n), sib]
    for dev in partners:
        pl.semaphore_signal(bar, inc=1, device_id=dev, device_id_type=MESH)

    cq = pltpu.make_async_copy(ql_hbm.at[0], qown.at[:, pl.ds(0, lat_w)], loc.at[0])
    cs = pltpu.make_async_copy(qr_hbm.at[0], qrv, loc.at[1])
    ct = pltpu.make_async_copy(pt_hbm, ptv, loc.at[2])
    cl = pltpu.make_async_copy(lat_hbm, lat, loc.at[3])
    cr = pltpu.make_async_copy(rope_hbm, rope, loc.at[4])
    ct.start()
    cs.start()
    cq.start()
    cl.start()
    cr.start()

    ct.wait()
    rows_t = []
    lane1 = lax.broadcasted_iota(jnp.int32, (1, 128), 1)
    entries = ptv.shape[1] // 128
    for r in range(entries):
        v = ptv[:, r * 128 : (r + 1) * 128]
        live = jnp.clip(len_ref[0] - (lane1 + r * 128) * page, 0, page)
        rows_t.append(jnp.where(v >= 0, v * 256 + live, -1))
    rows_t.append(jnp.full((8 - entries, 128), -1, jnp.int32))
    town[...] = jnp.concatenate(rows_t, axis=0)
    cs.wait()
    qown[:, pl.ds(lat_w, STAT)] = jnp.concatenate(
        [qrv[...], jnp.zeros((heads, STAT - rope_w), bf16)], axis=1
    )
    cq.wait()

    pl.semaphore_wait(bar, len(partners))

    for k in far:
        dev = at((x + k * (1 - c)) % n, (y + k * c) % n, 1)
        send(qown, QB.at[c, b, a], a_send.at[k], a_recv.at[c, k], dev)
    for k in far:
        send(town, TB.at[c, y], t_send.at[k], t_recv.at[c, k], at(x, (y + k) % n, 1))

    def part_of(par, idx, p):
        return QB.at[par, idx, pl.ds(p * per, per)]

    order = (
        tuple(range(SUBS)),
        tuple(range(SUBS // 2, SUBS)) + tuple(range(SUBS // 2)),
    )
    mid = (y, x)

    def origin(par, d, k):
        return (mid[par] + n - k) % n if d == 0 else (mid[par] + k) % n

    def subs_at(k):
        return SUBS // 2 if k == half else SUBS

    def build_table():
        first = (sq * n + x) * slots * 256
        codes = TB[...].reshape(n * 16, 128)
        ok = (codes >= first) & (codes < first + slots * 256)
        key = jnp.where(ok, codes - first, -1).T
        keys = [key] + [pltpu.roll(key, 128 - r, 1) for r in range(1, entries)]
        row = lax.broadcasted_iota(jnp.int32, (8, 128), 0)
        res = jnp.full((8, 128), -1, jnp.int32)
        for j in range(MOST):
            m = functools.reduce(jnp.maximum, keys)
            size = m.shape[0]
            while size > 8:
                size //= 2
                m = jnp.maximum(m[:size], m[size:])
            for r in (4, 2, 1):
                m = jnp.maximum(m, pltpu.roll(m, r, 0))
            res = jnp.where(row == j, m, res)
            full = jnp.concatenate([m] * (n * 2), axis=0)
            keys = [jnp.where(v == full, -1, v) for v in keys]
        tvm[...] = res
        cp = pltpu.make_async_copy(tvm, tsm, loc.at[5])
        cp.start()
        return cp

    def stats(top, total):
        hi = total.astype(bf16)
        lo = (total - hi.astype(f32)).astype(bf16)
        lane = lax.broadcasted_iota(jnp.int32, top.shape, 1)
        st = jnp.where(lane == 0, top, jnp.where(lane == 1, hi.astype(f32), lo.astype(f32)))
        return st.astype(bf16)

    def attend(par, yy):
        q = (QB[0, yy] if par == 0 else QB[1, :, yy]).reshape(n * heads, -1)
        ql, qr = q[:, :lat_w], q[:, lat_w : lat_w + rope_w]
        pages, ropes, counts = [], [], []
        for j in range(MOST):
            code = tsm[j, 8 * (par * n + yy)]
            slot = jnp.maximum(code, 0) // 256
            counts.append(jnp.where(code < 0, 0, code % 256))
            pages.append(lat[slot])
            ropes.append(rope[slot])
        keys = jnp.concatenate(pages, axis=0)
        sc = lax.dot_general(ql, keys, (((1,), (1,)), ((), ())), preferred_element_type=f32)
        sc = sc + jnp.dot(qr, jnp.concatenate(ropes, axis=1), preferred_element_type=f32)
        lane = lax.broadcasted_iota(jnp.int32, (n * heads, page), 1)
        live = [lane < v for v in counts]
        parts = [
            jnp.where(live[j], sc[:, j * page : (j + 1) * page] * softmax_scale, floor_score)
            for j in range(MOST)
        ]
        top = functools.reduce(jnp.maximum, parts)
        top = jnp.max(top, axis=1, keepdims=True).astype(bf16).astype(f32)
        ws = [jnp.where(o, jnp.exp(s - top), 0.0) for o, s in zip(live, parts)]
        total = jnp.sum(ws[0] + ws[1] + ws[2] + ws[3], axis=1, keepdims=True)
        w = jnp.concatenate([v.astype(bf16) for v in ws], axis=1)
        mixed = jnp.dot(w, keys, preferred_element_type=f32)
        top = jnp.broadcast_to(top, (n * heads, STAT))
        total = jnp.broadcast_to(total, (n * heads, STAT))
        return mixed, top, total

    def keep(par, yy, own, state):
        mixed, top, total = state
        shape = (n, heads, -1)

        if own and par == 0:
            LM[yy] = mixed.reshape(shape)
            LT[yy] = top.reshape(shape)
            LS[yy] = total.reshape(shape)
        elif own:
            LM[:, yy] = mixed.reshape(shape)
            LT[:, yy] = top.reshape(shape)
            LS[:, yy] = total.reshape(shape)
        else:
            full = jnp.concatenate([mixed.astype(bf16), stats(top, total)], axis=1)
            SB[yy] = full.reshape(shape)

    def push(par, yy):
        dst = RB.at[yy] if par == 0 else RB.at[:, yy]
        rcopy(SB.at[yy], dst, p_send.at[yy], p_recv.at[yy], sib).start()

    def compute(par, own, *seqs):
        states = [attend(par, yy) for yy in seqs]
        for yy, state in zip(seqs, states):
            keep(par, yy, own, state)
        if not own:
            for yy in seqs:
                push(par, yy)

    rows = per * heads
    er = lax.broadcasted_iota(jnp.int32, (STAT, 2 * STAT), 0)
    ec = lax.broadcasted_iota(jnp.int32, (STAT, 2 * STAT), 1)
    spread = jnp.where(
        ((er == 0) & (ec < STAT)) | ((er > 0) & (er < 3) & (ec >= STAT)), 1.0, 0.0
    ).astype(bf16)

    def opened(v):
        s = jnp.dot(v[:, lat_w:], spread, preferred_element_type=f32)
        tiles = [v[:, j * 128 : (j + 1) * 128].astype(f32) for j in range(lanes)]
        return tiles, s[:, :STAT], s[:, STAT:]

    def merge(states):
        top = functools.reduce(jnp.maximum, [s[1] for s in states])
        fac = [jnp.exp(s[1] - top) for s in states]
        total = sum(f * s[2] for f, s in zip(fac, states))
        tiles = [sum(f * s[0][j] for f, s in zip(fac, states)) for j in range(lanes)]
        return tiles, top, total

    def packed(state):
        tiles, top, total = state
        return jnp.concatenate([t.astype(bf16) for t in tiles] + [stats(top, total)], axis=1)

    def ps(p):
        return pl.ds(p * per, per)

    def both(idx, p):
        v = LM[idx, ps(p)].reshape(rows, lat_w)
        tiles = [v[:, j * 128 : (j + 1) * 128] for j in range(lanes)]
        top = LT[idx, ps(p)].reshape(rows, STAT)
        total = LS[idx, ps(p)].reshape(rows, STAT)
        return [(tiles, top, total), opened(RB[idx, ps(p)].reshape(rows, -1))]

    def goal(d, k):
        return (b + k) % n if d == 0 else (b + n - k) % n

    nxt = (dev_b((b + 1) % n), dev_b((b + n - 1) % n))
    halves = (
        (tuple(range(SUBS // 2, SUBS)), tuple(range(SUBS // 2))),
        (tuple(range(SUBS // 2)), tuple(range(SUBS // 2, SUBS))),
    )

    def reduce():
        out = []

        def put(src, dst, ss, rs, dev):
            cp = rcopy(src, dst, ss, rs, dev)
            cp.start()
            out.append(cp)

        def index(k, p):
            return p % (SUBS // 2) if k == 1 else SUBS // 2 + (k - 2) * SUBS + p

        def wait(d, k, p):
            i = index(k, p)
            part = RR.at[d, i]
            rcopy(part, part, r_send.at[d, i], r_recv.at[d, i], sib).wait_recv()

        def got(d, k, p):
            return [opened(RR[d, index(k, p)].reshape(rows, -1))]

        def step(k, subs, arrives):
            states = [both(goal(d, half + 1 - k), subs[d]) for d in range(2)]
            if arrives:
                for d in range(2):
                    wait(d, k - 1, subs[d])
                states = [states[d] + got(d, k - 1, subs[d]) for d in range(2)]
            full = [packed(merge(v)) for v in states]
            for d in range(2):
                MS[d, index(k, subs[d])] = full[d].reshape(per, heads, -1)
            for d in range(2):
                i = index(k, subs[d])
                put(MS.at[d, i], RR.at[d, i], r_send.at[d, i], r_recv.at[d, i], nxt[d])

        for i in range(n):
            rcopy(RB.at[i], RB.at[i], p_send.at[i], p_recv.at[i], sib).wait_recv()
        first, late = [tuple(zip(halves[0][h], halves[1][h])) for h in range(2)]
        for subs in late:
            step(1, subs, False)
        for subs in first:
            step(2, subs, False)
        for subs in late:
            step(2, subs, True)
        for k in range(3, half + 1):
            for subs in first + late:
                step(k, subs, True)
        for j in range(0, SUBS, 2):
            states = [both(b, p) for p in (j, j + 1)]
            for p in (j, j + 1):
                for d in range(2):
                    wait(d, half, p)
            full = [
                packed(merge(v + got(0, half, p) + got(1, half, p)))
                for v, p in zip(states, (j, j + 1))
            ]
            for v, p in zip(full, (j, j + 1)):
                M2[ps(p)] = v.reshape(per, heads, -1)
        for k in far:
            o = (a + k) % n
            put(M2.at[o], FB.at[k], f_send.at[k], f_recv.at[k], dev_a(o))
        for k in far:
            rcopy(FB.at[k], FB.at[k], f_send.at[k], f_recv.at[k], sib).wait_recv()
        tiles, top, total = merge([opened(M2[a])] + [opened(FB[k]) for k in far])
        out_ref[...] = jnp.concatenate([(t / total).astype(bf16) for t in tiles], axis=1)
        for i in range(n):
            rcopy(SB.at[i], SB.at[i], p_send.at[i], p_recv.at[i], sib).wait_send()
        for cp in out:
            cp.wait_send()

    @pl.when(c == 1)
    def _():
        out = []

        def put(src, dst, ss, rs, dev):
            cp = rcopy(src, dst, ss, rs, dev)
            cp.start()
            out.append(cp)

        neighbour = (
            (at(x, (y + 1) % n, 1), at(x, (y + n - 1) % n, 1)),
            (at((x + 1) % n, y, 1), at((x + n - 1) % n, y, 1)),
        )
        QB[1, x, y] = qown[...]
        TB[1, y] = town[...]
        for par in (1, 0):
            for k in far + ([0] if par == 0 else []):
                src = (x + n - k) % n if par == 0 else (y + n - k) % n
                part = QB.at[par, mid[par], src]
                rcopy(part, part, a_send.at[k], a_recv.at[par, k], sib).wait_recv()
            for j in range(SUBS):
                for d in range(2):
                    p = order[d][j]
                    part = part_of(par, mid[par], p)
                    put(part, part, g_send.at[par, d, p], g_recv.at[par, d, p], neighbour[par][d])
            part = QB.at[par, mid[par]]
            put(part, part, o_send.at[par], o_recv.at[par], sib)
        def ring_sub(k, j):
            for par in (1, 0):
                for d in range(2):
                    p = order[d][j]
                    i = (k - 1) * SUBS + p
                    part = part_of(par, origin(par, d, k), p)
                    rcopy(part, part, g_send.at[par, d, i], g_recv.at[par, d, i], sib).wait_recv()
                    if k < half - 1 or (k == half - 1 and j < SUBS // 2):
                        i2 = i + SUBS
                        ss, rs = g_send.at[par, d, i2], g_recv.at[par, d, i2]
                        put(part, part, ss, rs, neighbour[par][d])
                    put(part, part, d_send.at[par, d, i], d_recv.at[par, d, i], sib)

        def ring_all(k):
            for j in range(subs_at(k)):
                ring_sub(k, j)

        for par in (1, 0):
            for k in far + ([0] if par == 0 else []):
                part = TB.at[par, (y + n - k) % n]
                rcopy(part, part, t_send.at[k], t_recv.at[par, k], sib).wait_recv()
        put(TB, TB, o_send.at[2], o_recv.at[2], sib)
        built = build_table()
        cl.wait()
        cr.wait()
        built.wait()
        compute(0, False, y)
        ring_all(1)
        compute(0, False, (y + 1) % n)
        ring_all(2)
        compute(0, False, (y + n - 1) % n)
        ring_all(3)
        compute(0, False, (y + 2) % n)
        ring_all(half)
        compute(0, False, (y + n - 2) % n, (y + half) % n)
        compute(0, False, (y + n - 3) % n, (y + 3) % n)

        def odd(i, carry):
            compute(1, True, 2 * i, 2 * i + 1)
            return carry

        lax.fori_loop(0, n // 2, odd, 0)
        reduce()
        for cp in out:
            cp.wait_send()

    @pl.when(c == 0)
    def _():
        put_a = rcopy(qown, QB.at[0, y, x], a_send.at[0], a_recv.at[0, 0], sib)
        put_t = rcopy(town, TB.at[0, y], t_send.at[0], t_recv.at[0, 0], sib)
        put_a.start()
        put_t.start()

        def arrived(par, k):
            if k == 0:
                part = QB.at[par, mid[par]]
                rcopy(part, part, o_send.at[par], o_recv.at[par], sib).wait_recv()
                return
            for j in range(subs_at(k)):
                for d in range(2):
                    p = order[d][j]
                    i = (k - 1) * SUBS + p
                    part = part_of(par, origin(par, d, k), p)
                    rcopy(part, part, d_send.at[par, d, i], d_recv.at[par, d, i], sib).wait_recv()

        rcopy(TB, TB, o_send.at[2], o_recv.at[2], sib).wait_recv()
        built = build_table()
        cl.wait()
        cr.wait()
        arrived(0, 0)
        built.wait()
        compute(0, True, y)
        for k in range(1, half + 1):
            arrived(0, k)
            if k < half:
                compute(0, True, (y + n - k) % n, (y + k) % n)
            else:
                compute(0, True, (y + half) % n)
        for k in range(half + 1):
            arrived(1, k)

        def odd(i, carry):
            compute(1, False, 2 * i, 2 * i + 1)
            return carry

        lax.fori_loop(0, n // 2, odd, 0)
        reduce()
        put_a.wait_send()
        put_t.wait_send()

    for cp in sends:
        cp.wait_send()


def on_device(n, q_latent, q_rope, cache_latent, cache_rope, page_table, lengths):
    heads, lat_w = q_latent.shape[1:]
    rope_w = q_rope.shape[2]
    slots, page, _ = cache_latent.shape
    width = lat_w + STAT
    half, per = n // 2, n // SUBS
    messages = (half - 1) * SUBS + SUBS // 2
    any_spec = pl.BlockSpec(memory_space=pl.ANY)
    dma = pltpu.SemaphoreType.DMA
    out = pl.pallas_call(
        functools.partial(kernel, n, heads, lat_w, rope_w, page, slots),
        out_shape=jax.ShapeDtypeStruct((heads, lat_w), bf16),
        in_specs=[any_spec] * 5 + [pl.BlockSpec(memory_space=pltpu.SMEM)],
        out_specs=pl.BlockSpec(memory_space=pltpu.VMEM),
        scratch_shapes=[
            pltpu.VMEM(cache_latent.shape, bf16),
            pltpu.VMEM(cache_rope.shape, bf16),
            pltpu.VMEM((2, n, n, heads, width), bf16),
            pltpu.VMEM((2, n, 8, 128), jnp.int32),
            pltpu.VMEM((n, n, heads, width), bf16),
            pltpu.VMEM((n, n, heads, width), bf16),
            pltpu.VMEM((n, n, heads, lat_w), f32),
            pltpu.VMEM((n, n, heads, STAT), f32),
            pltpu.VMEM((n, n, heads, STAT), f32),
            pltpu.VMEM((2, messages, per, heads, width), bf16),
            pltpu.VMEM((2, messages, per, heads, width), bf16),
            pltpu.VMEM((n, heads, width), bf16),
            pltpu.VMEM((n, heads, width), bf16),
            pltpu.VMEM((heads, width), bf16),
            pltpu.VMEM((8, 128), jnp.int32),
            pltpu.VMEM((heads, rope_w), bf16),
            pltpu.VMEM(page_table.shape, jnp.int32),
            pltpu.VMEM((8, 128), jnp.int32),
            pltpu.SMEM((8, 128), jnp.int32),
            dma((6,)),
            dma((n,)), dma((2, n)), dma((n,)), dma((2, n)),
            dma((2, 2, half * SUBS)), dma((2, 2, half * SUBS)),
            dma((2, 2, half * SUBS)), dma((2, 2, half * SUBS)),
            dma((3,)), dma((3,)),
            dma((n,)), dma((n,)),
            dma((2, messages)), dma((2, messages)),
            dma((n,)), dma((n,)),
        ],
        compiler_params=pltpu.CompilerParams(
            collective_id=0, has_side_effects=True, vmem_limit_bytes=57 * 1024 * 1024
        ),
    )(q_latent, q_rope, cache_latent, cache_rope, page_table, lengths)
    return out[None]


def solution(mesh):
    n = mesh.shape["head"]
    assert n == 8 and mesh.shape["seq"] == 2 * n
    placed = (
        P(("grp", "seq"), "head", None),
        P(("grp", "seq"), "head", None),
        P(("grp", "seq", "head"), None, None),
        P(("grp", "seq", "head"), None, None),
        P(("grp", "seq"), None),
        P(("grp", "seq")),
    )
    return jax.shard_map(
        functools.partial(on_device, n),
        mesh=mesh,
        in_specs=placed,
        out_specs=P(("grp", "seq"), "head", None),
        check_vma=False,
    )
```

```python
import functools

import jax
import jax.numpy as jnp
from jax import lax
from jax.experimental import pallas as pl
from jax.experimental.pallas import tpu as pltpu
from jax.sharding import PartitionSpec as P

softmax_scale = 0.13528
floor_score = -1e30
MESH = pl.DeviceIdType.MESH
MOST = 4
STAT = 128
SUBS = 4
bf16, f32 = jnp.bfloat16, jnp.float32


def kernel(
    n, heads, lat_w, rope_w, page, slots,
    ql_hbm, qr_hbm, lat_hbm, rope_hbm, pt_hbm, len_ref,
    out_ref,
    lat, rope, QB, TB, SB, RB, LM, LT, LS, RR, MS, M2, FB, qown, town, qrv, ptv, tvm, tsm,
    loc, a_send, a_recv, t_send, t_recv, g_send, g_recv, d_send, d_recv, o_send, o_recv,
    p_send, p_recv, r_send, r_recv, f_send, f_recv,
):
    half = n // 2
    per = n // SUBS
    lanes = lat_w // 128
    sq = lax.axis_index("seq")
    x = lax.axis_index("head")
    y = sq // 2
    c = sq % 2
    a = x * (1 - c) + y * c
    b = y * (1 - c) + x * c

    def at(xx, yy, cc):
        return {"seq": 2 * yy + cc, "head": xx}

    def dev_a(i):
        return at(i * (1 - c) + x * c, y * (1 - c) + i * c, c)

    def dev_b(i):
        return at(x * (1 - c) + i * c, i * (1 - c) + y * c, c)

    sib = at(x, y, 1 - c)

    def rcopy(src, dst, ss, rs, dev):
        return pltpu.make_async_remote_copy(
            src_ref=src, dst_ref=dst, send_sem=ss, recv_sem=rs, device_id=dev, device_id_type=MESH
        )

    sends = []

    def send(src, dst, ss, rs, dev):
        cp = rcopy(src, dst, ss, rs, dev)
        cp.start()
        sends.append(cp)

    bar = pltpu.get_barrier_semaphore()
    far = sorted(range(1, n), key=lambda k: -min(k, n - k))
    partners = [at((x + k) % n, y, 1 - c) for k in far]
    partners += [at(x, (y + k) % n, 1 - c) for k in far]
    partners += [dev_a((a + k) % n) for k in far]
    partners += [dev_b((b + k) % n) for k in (1, 2, n - 2, n - 1)] + [sib]
    for dev in partners:
        pl.semaphore_signal(bar, inc=1, device_id=dev, device_id_type=MESH)

    cq = pltpu.make_async_copy(ql_hbm.at[0], qown.at[:, pl.ds(0, lat_w)], loc.at[0])
    cs = pltpu.make_async_copy(qr_hbm.at[0], qrv, loc.at[1])
    ct = pltpu.make_async_copy(pt_hbm, ptv, loc.at[2])
    cl = pltpu.make_async_copy(lat_hbm, lat, loc.at[3])
    cr = pltpu.make_async_copy(rope_hbm, rope, loc.at[4])
    ct.start()
    cs.start()
    cq.start()
    cl.start()
    cr.start()

    ct.wait()
    rows_t = []
    lane1 = lax.broadcasted_iota(jnp.int32, (1, 128), 1)
    entries = ptv.shape[1] // 128
    for r in range(entries):
        v = ptv[:, r * 128 : (r + 1) * 128]
        live = jnp.clip(len_ref[0] - (lane1 + r * 128) * page, 0, page)
        rows_t.append(jnp.where(v >= 0, v * 256 + live, -1))
    rows_t.append(jnp.full((8 - entries, 128), -1, jnp.int32))
    town[...] = jnp.concatenate(rows_t, axis=0)
    cs.wait()
    qown[:, pl.ds(lat_w, STAT)] = jnp.concatenate(
        [qrv[...], jnp.zeros((heads, STAT - rope_w), bf16)], axis=1
    )
    cq.wait()

    pl.semaphore_wait(bar, len(partners))

    for k in far:
        dev = at((x + k * (1 - c)) % n, (y + k * c) % n, 1)
        send(qown, QB.at[c, b, a], a_send.at[k], a_recv.at[c, k], dev)
    for k in far:
        send(town, TB.at[c, y], t_send.at[k], t_recv.at[c, k], at(x, (y + k) % n, 1))

    def part_of(par, idx, p):
        return QB.at[par, idx, pl.ds(p * per, per)]

    order = (
        tuple(range(SUBS)),
        tuple(range(SUBS // 2, SUBS)) + tuple(range(SUBS // 2)),
    )
    mid = (y, x)

    def origin(par, d, k):
        return (mid[par] + n - k) % n if d == 0 else (mid[par] + k) % n

    def subs_at(k):
        return SUBS // 2 if k == half else SUBS

    def build_table():
        first = (sq * n + x) * slots * 256
        codes = TB[...].reshape(n * 16, 128)
        ok = (codes >= first) & (codes < first + slots * 256)
        key = jnp.where(ok, codes - first, -1).T
        keys = [key] + [pltpu.roll(key, 128 - r, 1) for r in range(1, entries)]
        row = lax.broadcasted_iota(jnp.int32, (8, 128), 0)
        res = jnp.full((8, 128), -1, jnp.int32)
        for j in range(MOST):
            m = functools.reduce(jnp.maximum, keys)
            size = m.shape[0]
            while size > 8:
                size //= 2
                m = jnp.maximum(m[:size], m[size:])
            for r in (4, 2, 1):
                m = jnp.maximum(m, pltpu.roll(m, r, 0))
            res = jnp.where(row == j, m, res)
            full = jnp.concatenate([m] * (n * 2), axis=0)
            keys = [jnp.where(v == full, -1, v) for v in keys]
        tvm[...] = res
        cp = pltpu.make_async_copy(tvm, tsm, loc.at[5])
        cp.start()
        return cp

    def stats(top, total):
        hi = total.astype(bf16)
        lo = (total - hi.astype(f32)).astype(bf16)
        lane = lax.broadcasted_iota(jnp.int32, top.shape, 1)
        st = jnp.where(lane == 0, top, jnp.where(lane == 1, hi.astype(f32), lo.astype(f32)))
        return st.astype(bf16)

    def attend(par, yy):
        q = (QB[0, yy] if par == 0 else QB[1, :, yy]).reshape(n * heads, -1)
        ql, qr = q[:, :lat_w], q[:, lat_w : lat_w + rope_w]
        pages, ropes, counts = [], [], []
        for j in range(MOST):
            code = tsm[j, 8 * (par * n + yy)]
            slot = jnp.maximum(code, 0) // 256
            counts.append(jnp.where(code < 0, 0, code % 256))
            pages.append(lat[slot])
            ropes.append(rope[slot])
        keys = jnp.concatenate(pages, axis=0)
        sc = lax.dot_general(ql, keys, (((1,), (1,)), ((), ())), preferred_element_type=f32)
        sc = sc + jnp.dot(qr, jnp.concatenate(ropes, axis=1), preferred_element_type=f32)
        lane = lax.broadcasted_iota(jnp.int32, (n * heads, page), 1)
        live = [lane < v for v in counts]
        parts = [
            jnp.where(live[j], sc[:, j * page : (j + 1) * page] * softmax_scale, floor_score)
            for j in range(MOST)
        ]
        top = functools.reduce(jnp.maximum, parts)
        top = jnp.max(top, axis=1, keepdims=True).astype(bf16).astype(f32)
        ws = [jnp.where(o, jnp.exp(s - top), 0.0) for o, s in zip(live, parts)]
        total = jnp.sum(ws[0] + ws[1] + ws[2] + ws[3], axis=1, keepdims=True)
        w = jnp.concatenate([v.astype(bf16) for v in ws], axis=1)
        mixed = jnp.dot(w, keys, preferred_element_type=f32)
        top = jnp.broadcast_to(top, (n * heads, STAT))
        total = jnp.broadcast_to(total, (n * heads, STAT))
        return mixed, top, total

    def keep(par, yy, own, state):
        mixed, top, total = state
        shape = (n, heads, -1)

        if own and par == 0:
            LM[yy] = mixed.reshape(shape)
            LT[yy] = top.reshape(shape)
            LS[yy] = total.reshape(shape)
        elif own:
            LM[:, yy] = mixed.reshape(shape)
            LT[:, yy] = top.reshape(shape)
            LS[:, yy] = total.reshape(shape)
        else:
            full = jnp.concatenate([mixed.astype(bf16), stats(top, total)], axis=1)
            SB[yy] = full.reshape(shape)

    def push(par, yy):
        dst = RB.at[yy] if par == 0 else RB.at[:, yy]
        rcopy(SB.at[yy], dst, p_send.at[yy], p_recv.at[yy], sib).start()

    def compute(par, own, *seqs):
        states = [attend(par, yy) for yy in seqs]
        for yy, state in zip(seqs, states):
            keep(par, yy, own, state)
        if not own:
            for yy in seqs:
                push(par, yy)

    rows = per * heads
    er = lax.broadcasted_iota(jnp.int32, (STAT, 2 * STAT), 0)
    ec = lax.broadcasted_iota(jnp.int32, (STAT, 2 * STAT), 1)
    spread = jnp.where(
        ((er == 0) & (ec < STAT)) | ((er > 0) & (er < 3) & (ec >= STAT)), 1.0, 0.0
    ).astype(bf16)

    def opened(v):
        s = jnp.dot(v[:, lat_w:], spread, preferred_element_type=f32)
        tiles = [v[:, j * 128 : (j + 1) * 128].astype(f32) for j in range(lanes)]
        return tiles, s[:, :STAT], s[:, STAT:]

    def merge(states):
        top = functools.reduce(jnp.maximum, [s[1] for s in states])
        fac = [jnp.exp(s[1] - top) for s in states]
        total = sum(f * s[2] for f, s in zip(fac, states))
        tiles = [sum(f * s[0][j] for f, s in zip(fac, states)) for j in range(lanes)]
        return tiles, top, total

    def packed(state):
        tiles, top, total = state
        return jnp.concatenate([t.astype(bf16) for t in tiles] + [stats(top, total)], axis=1)

    def ps(p):
        return pl.ds(p * per, per)

    def both(idx, p):
        v = LM[idx, ps(p)].reshape(rows, lat_w)
        tiles = [v[:, j * 128 : (j + 1) * 128] for j in range(lanes)]
        top = LT[idx, ps(p)].reshape(rows, STAT)
        total = LS[idx, ps(p)].reshape(rows, STAT)
        return [(tiles, top, total), opened(RB[idx, ps(p)].reshape(rows, -1))]

    def goal(d, k):
        return (b + k) % n if d == 0 else (b + n - k) % n

    halves = (
        (tuple(range(SUBS // 2, SUBS)), tuple(range(SUBS // 2))),
        (tuple(range(SUBS // 2)), tuple(range(SUBS // 2, SUBS))),
    )

    def reduce(gap):
        out = []

        def put(src, dst, ss, rs, dev):
            cp = rcopy(src, dst, ss, rs, dev)
            cp.start()
            out.append(cp)

        def index(k, p):
            return {4: p % (SUBS // 2), 3: SUBS // 2, 2: SUBS // 2 + SUBS, 1: SUBS // 2 + 2 * SUBS}[
                k
            ] + (p if k < half else 0)

        def wait(d, k, p):
            i = index(k, p)
            part = RR.at[d, i]
            rcopy(part, part, r_send.at[d, i], r_recv.at[d, i], sib).wait_recv()

        def got(d, k, p):
            return [opened(RR[d, index(k, p)].reshape(rows, -1))]

        def step(k, subs, comes=()):
            states = [both(goal(d, k), subs[d]) for d in range(2)]
            for d in range(2):
                for g in comes:
                    wait(d, g, subs[d])
            for g in comes:
                states = [states[d] + got(d, g, subs[d]) for d in range(2)]
            full = [packed(merge(v)) for v in states]
            for d in range(2):
                MS[d, index(k, subs[d])] = full[d].reshape(per, heads, -1)
            for d in range(2):
                i, hops = index(k, subs[d]), 2 - k % 2
                dev = dev_b((b + (hops if d == 0 else n - hops)) % n)
                put(MS.at[d, i], RR.at[d, i], r_send.at[d, i], r_recv.at[d, i], dev)

        for i in range(n):
            rcopy(RB.at[i], RB.at[i], p_send.at[i], p_recv.at[i], sib).wait_recv()
        first, late = [tuple(zip(halves[0][h], halves[1][h])) for h in range(2)]
        for subs in late:
            step(4, subs)
        for subs in first + late:
            step(3, subs)
        for subs in first + late:
            step(1, subs)
        gap()
        for subs in first:
            step(2, subs, (3,))
        for subs in late:
            step(2, subs, (3, 4))
        for j in range(0, SUBS, 2):
            states = [both(b, p) for p in (j, j + 1)]
            for k in (1, 2):
                for p in (j, j + 1):
                    for d in range(2):
                        wait(d, k, p)
            full = [
                packed(merge(v + [g for k in (1, 2) for d in range(2) for g in got(d, k, p)]))
                for v, p in zip(states, (j, j + 1))
            ]
            for v, p in zip(full, (j, j + 1)):
                M2[ps(p)] = v.reshape(per, heads, -1)
        for k in far:
            o = (a + k) % n
            put(M2.at[o], FB.at[k], f_send.at[k], f_recv.at[k], dev_a(o))
        for k in far:
            rcopy(FB.at[k], FB.at[k], f_send.at[k], f_recv.at[k], sib).wait_recv()
        tiles, top, total = merge([opened(M2[a])] + [opened(FB[k]) for k in far])
        out_ref[...] = jnp.concatenate([(t / total).astype(bf16) for t in tiles], axis=1)
        for i in range(n):
            rcopy(SB.at[i], SB.at[i], p_send.at[i], p_recv.at[i], sib).wait_send()
        for cp in out:
            cp.wait_send()

    @pl.when(c == 1)
    def _():
        out = []

        def put(src, dst, ss, rs, dev):
            cp = rcopy(src, dst, ss, rs, dev)
            cp.start()
            out.append(cp)

        neighbour = (
            (at(x, (y + 1) % n, 1), at(x, (y + n - 1) % n, 1)),
            (at((x + 1) % n, y, 1), at((x + n - 1) % n, y, 1)),
        )
        QB[1, x, y] = qown[...]
        TB[1, y] = town[...]
        for par in (1, 0):
            for k in far + ([0] if par == 0 else []):
                src = (x + n - k) % n if par == 0 else (y + n - k) % n
                part = QB.at[par, mid[par], src]
                rcopy(part, part, a_send.at[k], a_recv.at[par, k], sib).wait_recv()
            for j in range(SUBS):
                for d in range(2):
                    p = order[d][j]
                    part = part_of(par, mid[par], p)
                    put(part, part, g_send.at[par, d, p], g_recv.at[par, d, p], neighbour[par][d])
            part = QB.at[par, mid[par]]
            put(part, part, o_send.at[par], o_recv.at[par], sib)
        def ring_sub(k, j):
            for par in (1, 0):
                for d in range(2):
                    p = order[d][j]
                    i = (k - 1) * SUBS + p
                    part = part_of(par, origin(par, d, k), p)
                    rcopy(part, part, g_send.at[par, d, i], g_recv.at[par, d, i], sib).wait_recv()
                    if k < half - 1 or (k == half - 1 and j < SUBS // 2):
                        i2 = i + SUBS
                        ss, rs = g_send.at[par, d, i2], g_recv.at[par, d, i2]
                        put(part, part, ss, rs, neighbour[par][d])
                    put(part, part, d_send.at[par, d, i], d_recv.at[par, d, i], sib)

        def ring_all(k):
            for j in range(subs_at(k)):
                ring_sub(k, j)

        for par in (1, 0):
            for k in far + ([0] if par == 0 else []):
                part = TB.at[par, (y + n - k) % n]
                rcopy(part, part, t_send.at[k], t_recv.at[par, k], sib).wait_recv()
        put(TB, TB, o_send.at[2], o_recv.at[2], sib)
        built = build_table()
        cl.wait()
        cr.wait()
        built.wait()
        compute(0, False, y)
        ring_all(1)
        compute(0, False, (y + 1) % n)
        ring_all(2)
        compute(0, False, (y + n - 1) % n)
        ring_all(3)
        compute(0, False, (y + 2) % n)
        ring_all(half)
        compute(0, False, (y + n - 2) % n, (y + half) % n)
        compute(0, False, (y + n - 3) % n, (y + 3) % n)

        def odd(i, carry):
            compute(1, True, 2 * i, 2 * i + 1)
            return carry

        lax.fori_loop(0, n // 2, odd, 0)
        reduce(lambda: None)
        for cp in out:
            cp.wait_send()

    @pl.when(c == 0)
    def _():
        put_a = rcopy(qown, QB.at[0, y, x], a_send.at[0], a_recv.at[0, 0], sib)
        put_t = rcopy(town, TB.at[0, y], t_send.at[0], t_recv.at[0, 0], sib)
        put_a.start()
        put_t.start()

        def arrived(par, k):
            if k == 0:
                part = QB.at[par, mid[par]]
                rcopy(part, part, o_send.at[par], o_recv.at[par], sib).wait_recv()
                return
            for j in range(subs_at(k)):
                for d in range(2):
                    p = order[d][j]
                    i = (k - 1) * SUBS + p
                    part = part_of(par, origin(par, d, k), p)
                    rcopy(part, part, d_send.at[par, d, i], d_recv.at[par, d, i], sib).wait_recv()

        rcopy(TB, TB, o_send.at[2], o_recv.at[2], sib).wait_recv()
        built = build_table()
        cl.wait()
        cr.wait()
        arrived(0, 0)
        built.wait()
        compute(0, True, y)
        for k in range(1, half + 1):
            arrived(0, k)
            if k < half:
                compute(0, True, (y + n - k) % n, (y + k) % n)
            else:
                compute(0, True, (y + half) % n)
        for k in range(half + 1):
            arrived(1, k)

        def odd(i, carry):
            compute(1, False, 2 * i, 2 * i + 1)
            return carry

        lax.fori_loop(0, n // 2, odd, 0)
        reduce(lambda: None)
        put_a.wait_send()
        put_t.wait_send()

    for cp in sends:
        cp.wait_send()


def on_device(n, q_latent, q_rope, cache_latent, cache_rope, page_table, lengths):
    heads, lat_w = q_latent.shape[1:]
    rope_w = q_rope.shape[2]
    slots, page, _ = cache_latent.shape
    width = lat_w + STAT
    half, per = n // 2, n // SUBS
    messages = (half - 1) * SUBS + SUBS // 2
    any_spec = pl.BlockSpec(memory_space=pl.ANY)
    dma = pltpu.SemaphoreType.DMA
    out = pl.pallas_call(
        functools.partial(kernel, n, heads, lat_w, rope_w, page, slots),
        out_shape=pltpu.VMEM((heads, lat_w), bf16),
        in_specs=[any_spec] * 5 + [pl.BlockSpec(memory_space=pltpu.SMEM)],
        out_specs=pl.BlockSpec(memory_space=pltpu.VMEM),
        scratch_shapes=[
            pltpu.VMEM(cache_latent.shape, bf16),
            pltpu.VMEM(cache_rope.shape, bf16),
            pltpu.VMEM((2, n, n, heads, width), bf16),
            pltpu.VMEM((2, n, 8, 128), jnp.int32),
            pltpu.VMEM((n, n, heads, width), bf16),
            pltpu.VMEM((n, n, heads, width), bf16),
            pltpu.VMEM((n, n, heads, lat_w), f32),
            pltpu.VMEM((n, n, heads, STAT), f32),
            pltpu.VMEM((n, n, heads, STAT), f32),
            pltpu.VMEM((2, messages, per, heads, width), bf16),
            pltpu.VMEM((2, messages, per, heads, width), bf16),
            pltpu.VMEM((n, heads, width), bf16),
            pltpu.VMEM((n, heads, width), bf16),
            pltpu.VMEM((heads, width), bf16),
            pltpu.VMEM((8, 128), jnp.int32),
            pltpu.VMEM((heads, rope_w), bf16),
            pltpu.VMEM(page_table.shape, jnp.int32),
            pltpu.VMEM((8, 128), jnp.int32),
            pltpu.SMEM((8, 128), jnp.int32),
            dma((6,)),
            dma((n,)), dma((2, n)), dma((n,)), dma((2, n)),
            dma((2, 2, half * SUBS)), dma((2, 2, half * SUBS)),
            dma((2, 2, half * SUBS)), dma((2, 2, half * SUBS)),
            dma((3,)), dma((3,)),
            dma((n,)), dma((n,)),
            dma((2, messages)), dma((2, messages)),
            dma((n,)), dma((n,)),
        ],
        compiler_params=pltpu.CompilerParams(
            collective_id=0, has_side_effects=True, vmem_limit_bytes=57 * 1024 * 1024
        ),
    )(q_latent, q_rope, cache_latent, cache_rope, page_table, lengths)
    return out[None]


def solution(mesh):
    n = mesh.shape["head"]
    assert n == 8 and mesh.shape["seq"] == 2 * n
    placed = (
        P(("grp", "seq"), "head", None),
        P(("grp", "seq"), "head", None),
        P(("grp", "seq", "head"), None, None),
        P(("grp", "seq", "head"), None, None),
        P(("grp", "seq"), None),
        P(("grp", "seq")),
    )
    return jax.shard_map(
        functools.partial(on_device, n),
        mesh=mesh,
        in_specs=placed,
        out_specs=P(("grp", "seq"), "head", None),
        check_vma=False,
    )
```

```python
import functools

import jax
import jax.numpy as jnp
from jax import lax
from jax.experimental import pallas as pl
from jax.experimental.pallas import tpu as pltpu
from jax.sharding import PartitionSpec as P

softmax_scale = 0.13528
floor_score = -1e30
MESH = pl.DeviceIdType.MESH
MOST = 4
STAT = 128
SUBS = 4
GSUBS = 2
bf16, f32 = jnp.bfloat16, jnp.float32


def kernel(
    n, heads, lat_w, rope_w, page, slots,
    ql_hbm, qr_hbm, lat_hbm, rope_hbm, pt_hbm, len_ref,
    out_ref,
    lat, rope, QB, TB, SB, RB, LM, LT, LS, RR, MS, M2, FB, qown, town, qrv, ptv, tvm, tsm,
    loc, a_send, a_recv, t_send, t_recv, g_send, g_recv, d_send, d_recv, o_send, o_recv,
    p_send, p_recv, r_send, r_recv, f_send, f_recv,
):
    half = n // 2
    per = n // SUBS
    lanes = lat_w // 128
    sq = lax.axis_index("seq")
    x = lax.axis_index("head")
    y = sq // 2
    c = sq % 2
    a = x * (1 - c) + y * c
    b = y * (1 - c) + x * c

    def at(xx, yy, cc):
        return {"seq": 2 * yy + cc, "head": xx}

    def dev_a(i):
        return at(i * (1 - c) + x * c, y * (1 - c) + i * c, c)

    def dev_b(i):
        return at(x * (1 - c) + i * c, i * (1 - c) + y * c, c)

    sib = at(x, y, 1 - c)

    def rcopy(src, dst, ss, rs, dev):
        return pltpu.make_async_remote_copy(
            src_ref=src, dst_ref=dst, send_sem=ss, recv_sem=rs, device_id=dev, device_id_type=MESH
        )

    sends = []

    def send(src, dst, ss, rs, dev):
        cp = rcopy(src, dst, ss, rs, dev)
        cp.start()
        sends.append(cp)

    bar = pltpu.get_barrier_semaphore()
    far = sorted(range(1, n), key=lambda k: -min(k, n - k))
    partners = [at((x + k) % n, y, 1 - c) for k in far]
    partners += [at(x, (y + k) % n, 1 - c) for k in far]
    partners += [dev_a((a + k) % n) for k in far]
    partners += [dev_b((b + k) % n) for k in (1, 2, n - 2, n - 1)] + [sib]
    for dev in partners:
        pl.semaphore_signal(bar, inc=1, device_id=dev, device_id_type=MESH)

    cq = pltpu.make_async_copy(ql_hbm.at[0], qown.at[:, pl.ds(0, lat_w)], loc.at[0])
    cs = pltpu.make_async_copy(qr_hbm.at[0], qrv, loc.at[1])
    ct = pltpu.make_async_copy(pt_hbm, ptv, loc.at[2])
    cl = pltpu.make_async_copy(lat_hbm, lat, loc.at[3])
    cr = pltpu.make_async_copy(rope_hbm, rope, loc.at[4])
    ct.start()
    cs.start()
    cq.start()
    cl.start()
    cr.start()

    ct.wait()
    rows_t = []
    lane1 = lax.broadcasted_iota(jnp.int32, (1, 128), 1)
    entries = ptv.shape[1] // 128
    for r in range(entries):
        v = ptv[:, r * 128 : (r + 1) * 128]
        live = jnp.clip(len_ref[0] - (lane1 + r * 128) * page, 0, page)
        rows_t.append(jnp.where(v >= 0, v * 256 + live, -1))
    rows_t.append(jnp.full((8 - entries, 128), -1, jnp.int32))
    town[...] = jnp.concatenate(rows_t, axis=0)
    cs.wait()
    qown[:, pl.ds(lat_w, STAT)] = jnp.concatenate(
        [qrv[...], jnp.zeros((heads, STAT - rope_w), bf16)], axis=1
    )
    cq.wait()

    pl.semaphore_wait(bar, len(partners))

    for k in far:
        dev = at((x + k * (1 - c)) % n, (y + k * c) % n, 1)
        send(qown, QB.at[c, b, a], a_send.at[k], a_recv.at[c, k], dev)
    for k in far:
        send(town, TB.at[c, y], t_send.at[k], t_recv.at[c, k], at(x, (y + k) % n, 1))

    def part_of(par, idx, p):
        return QB.at[par, idx, pl.ds(p * (n // GSUBS), n // GSUBS)]

    order = (
        tuple(range(GSUBS)),
        tuple(range(GSUBS // 2, GSUBS)) + tuple(range(GSUBS // 2)),
    )
    mid = (y, x)

    def origin(par, d, k):
        return (mid[par] + n - k) % n if d == 0 else (mid[par] + k) % n

    def subs_at(k):
        return GSUBS // 2 if k == half else GSUBS

    def build_table():
        first = (sq * n + x) * slots * 256
        codes = TB[...].reshape(n * 16, 128)
        ok = (codes >= first) & (codes < first + slots * 256)
        key = jnp.where(ok, codes - first, -1).T
        keys = [key] + [pltpu.roll(key, 128 - r, 1) for r in range(1, entries)]
        row = lax.broadcasted_iota(jnp.int32, (8, 128), 0)
        res = jnp.full((8, 128), -1, jnp.int32)
        for j in range(MOST):
            m = functools.reduce(jnp.maximum, keys)
            size = m.shape[0]
            while size > 8:
                size //= 2
                m = jnp.maximum(m[:size], m[size:])
            for r in (4, 2, 1):
                m = jnp.maximum(m, pltpu.roll(m, r, 0))
            res = jnp.where(row == j, m, res)
            full = jnp.concatenate([m] * (n * 2), axis=0)
            keys = [jnp.where(v == full, -1, v) for v in keys]
        tvm[...] = res
        cp = pltpu.make_async_copy(tvm, tsm, loc.at[5])
        cp.start()
        return cp

    def stats(top, total):
        hi = total.astype(bf16)
        lo = (total - hi.astype(f32)).astype(bf16)
        lane = lax.broadcasted_iota(jnp.int32, top.shape, 1)
        st = jnp.where(lane == 0, top, jnp.where(lane == 1, hi.astype(f32), lo.astype(f32)))
        return st.astype(bf16)

    def attend(par, yy):
        q = (QB[0, yy] if par == 0 else QB[1, :, yy]).reshape(n * heads, -1)
        ql, qr = q[:, :lat_w], q[:, lat_w : lat_w + rope_w]
        pages, ropes, counts = [], [], []
        for j in range(MOST):
            code = tsm[j, 8 * (par * n + yy)]
            slot = jnp.maximum(code, 0) // 256
            counts.append(jnp.where(code < 0, 0, code % 256))
            pages.append(lat[slot])
            ropes.append(rope[slot])
        keys = jnp.concatenate(pages, axis=0)
        sc = lax.dot_general(ql, keys, (((1,), (1,)), ((), ())), preferred_element_type=f32)
        sc = sc + jnp.dot(qr, jnp.concatenate(ropes, axis=1), preferred_element_type=f32)
        lane = lax.broadcasted_iota(jnp.int32, (n * heads, page), 1)
        live = [lane < v for v in counts]
        parts = [
            jnp.where(live[j], sc[:, j * page : (j + 1) * page] * softmax_scale, floor_score)
            for j in range(MOST)
        ]
        top = functools.reduce(jnp.maximum, parts)
        top = jnp.max(top, axis=1, keepdims=True).astype(bf16).astype(f32)
        ws = [jnp.where(o, jnp.exp(s - top), 0.0) for o, s in zip(live, parts)]
        total = jnp.sum(ws[0] + ws[1] + ws[2] + ws[3], axis=1, keepdims=True)
        w = jnp.concatenate([v.astype(bf16) for v in ws], axis=1)
        mixed = jnp.dot(w, keys, preferred_element_type=f32)
        top = jnp.broadcast_to(top, (n * heads, STAT))
        total = jnp.broadcast_to(total, (n * heads, STAT))
        return mixed, top, total

    def keep(par, yy, own, state):
        mixed, top, total = state
        shape = (n, heads, -1)

        if own and par == 0:
            LM[yy] = mixed.reshape(shape)
            LT[yy] = top.reshape(shape)
            LS[yy] = total.reshape(shape)
        elif own:
            LM[:, yy] = mixed.reshape(shape)
            LT[:, yy] = top.reshape(shape)
            LS[:, yy] = total.reshape(shape)
        else:
            full = jnp.concatenate([mixed.astype(bf16), stats(top, total)], axis=1)
            SB[yy] = full.reshape(shape)

    def push(par, yy):
        dst = RB.at[yy] if par == 0 else RB.at[:, yy]
        rcopy(SB.at[yy], dst, p_send.at[yy], p_recv.at[yy], sib).start()

    def compute(par, own, *seqs):
        states = [attend(par, yy) for yy in seqs]
        for yy, state in zip(seqs, states):
            keep(par, yy, own, state)
        if not own:
            for yy in seqs:
                push(par, yy)

    rows = per * heads
    er = lax.broadcasted_iota(jnp.int32, (STAT, 2 * STAT), 0)
    ec = lax.broadcasted_iota(jnp.int32, (STAT, 2 * STAT), 1)
    spread = jnp.where(
        ((er == 0) & (ec < STAT)) | ((er > 0) & (er < 3) & (ec >= STAT)), 1.0, 0.0
    ).astype(bf16)

    def opened(v):
        s = jnp.dot(v[:, lat_w:], spread, preferred_element_type=f32)
        tiles = [v[:, j * 128 : (j + 1) * 128].astype(f32) for j in range(lanes)]
        return tiles, s[:, :STAT], s[:, STAT:]

    def merge(states):
        top = functools.reduce(jnp.maximum, [s[1] for s in states])
        fac = [jnp.exp(s[1] - top) for s in states]
        total = sum(f * s[2] for f, s in zip(fac, states))
        tiles = [sum(f * s[0][j] for f, s in zip(fac, states)) for j in range(lanes)]
        return tiles, top, total

    def packed(state):
        tiles, top, total = state
        return jnp.concatenate([t.astype(bf16) for t in tiles] + [stats(top, total)], axis=1)

    def ps(p):
        return pl.ds(p * per, per)

    def both(idx, p):
        v = LM[idx, ps(p)].reshape(rows, lat_w)
        tiles = [v[:, j * 128 : (j + 1) * 128] for j in range(lanes)]
        top = LT[idx, ps(p)].reshape(rows, STAT)
        total = LS[idx, ps(p)].reshape(rows, STAT)
        return [(tiles, top, total), opened(RB[idx, ps(p)].reshape(rows, -1))]

    def goal(d, k):
        return (b + k) % n if d == 0 else (b + n - k) % n

    halves = (
        (tuple(range(SUBS // 2, SUBS)), tuple(range(SUBS // 2))),
        (tuple(range(SUBS // 2)), tuple(range(SUBS // 2, SUBS))),
    )

    def reduce(need):
        out = []

        def put(src, dst, ss, rs, dev):
            cp = rcopy(src, dst, ss, rs, dev)
            cp.start()
            out.append(cp)

        def index(k, p):
            return {4: p % (SUBS // 2), 3: SUBS // 2, 2: SUBS // 2 + SUBS, 1: SUBS // 2 + 2 * SUBS}[
                k
            ] + (p if k < half else 0)

        def wait(d, k, p):
            i = index(k, p)
            part = RR.at[d, i]
            rcopy(part, part, r_send.at[d, i], r_recv.at[d, i], sib).wait_recv()

        def got(d, k, p):
            return [opened(RR[d, index(k, p)].reshape(rows, -1))]

        def step(k, subs, comes=()):
            states = [both(goal(d, k), subs[d]) for d in range(2)]
            for d in range(2):
                for g in comes:
                    wait(d, g, subs[d])
            for g in comes:
                states = [states[d] + got(d, g, subs[d]) for d in range(2)]
            full = [packed(merge(v)) for v in states]
            for d in range(2):
                MS[d, index(k, subs[d])] = full[d].reshape(per, heads, -1)
            for d in range(2):
                i, hops = index(k, subs[d]), 2 - k % 2
                dev = dev_b((b + (hops if d == 0 else n - hops)) % n)
                put(MS.at[d, i], RR.at[d, i], r_send.at[d, i], r_recv.at[d, i], dev)

        first, late = [tuple(zip(halves[0][h], halves[1][h])) for h in range(2)]
        for j in range(2):
            for i in need[j]:
                rcopy(RB.at[i], RB.at[i], p_send.at[i], p_recv.at[i], sib).wait_recv()
            step(4, late[j])
            step(3, first[j])
            step(3, late[j])
            step(1, first[j])
            step(1, late[j])
        for subs in first:
            step(2, subs, (3,))
        for subs in late:
            step(2, subs, (3, 4))
        for j in range(0, SUBS, 2):
            states = [both(b, p) for p in (j, j + 1)]
            for k in (1, 2):
                for p in (j, j + 1):
                    for d in range(2):
                        wait(d, k, p)
            full = [
                packed(merge(v + [g for k in (1, 2) for d in range(2) for g in got(d, k, p)]))
                for v, p in zip(states, (j, j + 1))
            ]
            for v, p in zip(full, (j, j + 1)):
                M2[ps(p)] = v.reshape(per, heads, -1)
        for k in far:
            o = (a + k) % n
            put(M2.at[o], FB.at[k], f_send.at[k], f_recv.at[k], dev_a(o))
        for k in far:
            rcopy(FB.at[k], FB.at[k], f_send.at[k], f_recv.at[k], sib).wait_recv()
        tiles, top, total = merge([opened(M2[a])] + [opened(FB[k]) for k in far])
        out_ref[...] = jnp.concatenate([(t / total).astype(bf16) for t in tiles], axis=1)
        for i in range(n):
            rcopy(SB.at[i], SB.at[i], p_send.at[i], p_recv.at[i], sib).wait_send()
        for cp in out:
            cp.wait_send()

    @pl.when(c == 1)
    def _():
        out = []

        def put(src, dst, ss, rs, dev):
            cp = rcopy(src, dst, ss, rs, dev)
            cp.start()
            out.append(cp)

        neighbour = (
            (at(x, (y + 1) % n, 1), at(x, (y + n - 1) % n, 1)),
            (at((x + 1) % n, y, 1), at((x + n - 1) % n, y, 1)),
        )
        QB[1, x, y] = qown[...]
        TB[1, y] = town[...]
        for par in (1, 0):
            for k in far + ([0] if par == 0 else []):
                src = (x + n - k) % n if par == 0 else (y + n - k) % n
                part = QB.at[par, mid[par], src]
                rcopy(part, part, a_send.at[k], a_recv.at[par, k], sib).wait_recv()
            for j in range(GSUBS):
                for d in range(2):
                    p = order[d][j]
                    part = part_of(par, mid[par], p)
                    put(part, part, g_send.at[par, d, p], g_recv.at[par, d, p], neighbour[par][d])
            part = QB.at[par, mid[par]]
            put(part, part, o_send.at[par], o_recv.at[par], sib)
        def ring_sub(k, j):
            for par in (1, 0):
                for d in range(2):
                    p = order[d][j]
                    i = (k - 1) * GSUBS + p
                    part = part_of(par, origin(par, d, k), p)
                    rcopy(part, part, g_send.at[par, d, i], g_recv.at[par, d, i], sib).wait_recv()
                    if k < half - 1 or (k == half - 1 and j < GSUBS // 2):
                        i2 = i + GSUBS
                        ss, rs = g_send.at[par, d, i2], g_recv.at[par, d, i2]
                        put(part, part, ss, rs, neighbour[par][d])
                    put(part, part, d_send.at[par, d, i], d_recv.at[par, d, i], sib)

        def ring_all(k):
            for j in range(subs_at(k)):
                ring_sub(k, j)

        for par in (1, 0):
            for k in far + ([0] if par == 0 else []):
                part = TB.at[par, (y + n - k) % n]
                rcopy(part, part, t_send.at[k], t_recv.at[par, k], sib).wait_recv()
        put(TB, TB, o_send.at[2], o_recv.at[2], sib)
        built = build_table()
        cl.wait()
        cr.wait()
        built.wait()
        compute(0, False, y)
        ring_all(1)
        compute(0, False, (y + 1) % n)
        ring_all(2)
        compute(0, False, (y + n - 1) % n)
        ring_all(3)
        compute(0, False, (y + 2) % n)
        ring_all(half)
        compute(0, False, (y + n - 2) % n, (y + half) % n)
        compute(0, False, (y + n - 3) % n, (y + 3) % n)

        def odd(i, carry):
            first = 4 * (i % 2) + 2 * (i // 2)
            compute(1, True, first, first + 1)
            return carry

        lax.fori_loop(0, n // 2, odd, 0)
        reduce(((0, 1, 4, 5), (2, 3, 6, 7)))
        for cp in out:
            cp.wait_send()

    @pl.when(c == 0)
    def _():
        put_a = rcopy(qown, QB.at[0, y, x], a_send.at[0], a_recv.at[0, 0], sib)
        put_t = rcopy(town, TB.at[0, y], t_send.at[0], t_recv.at[0, 0], sib)
        put_a.start()
        put_t.start()

        def arrived(par, k):
            if k == 0:
                part = QB.at[par, mid[par]]
                rcopy(part, part, o_send.at[par], o_recv.at[par], sib).wait_recv()
                return
            for j in range(subs_at(k)):
                for d in range(2):
                    p = order[d][j]
                    i = (k - 1) * GSUBS + p
                    part = part_of(par, origin(par, d, k), p)
                    rcopy(part, part, d_send.at[par, d, i], d_recv.at[par, d, i], sib).wait_recv()

        rcopy(TB, TB, o_send.at[2], o_recv.at[2], sib).wait_recv()
        built = build_table()
        cl.wait()
        cr.wait()
        arrived(0, 0)
        built.wait()
        compute(0, True, y)
        for k in range(1, half + 1):
            arrived(0, k)
            if k < half:
                compute(0, True, (y + n - k) % n, (y + k) % n)
            else:
                compute(0, True, (y + half) % n)
        for k in range(half + 1):
            arrived(1, k)

        def odd(i, carry):
            first = 4 * (i % 2) + 2 * (i // 2)
            compute(1, False, first, first + 1)
            return carry

        lax.fori_loop(0, n // 2, odd, 0)
        reduce((tuple(range(n)), ()))
        put_a.wait_send()
        put_t.wait_send()

    for cp in sends:
        cp.wait_send()


def on_device(n, q_latent, q_rope, cache_latent, cache_rope, page_table, lengths):
    heads, lat_w = q_latent.shape[1:]
    rope_w = q_rope.shape[2]
    slots, page, _ = cache_latent.shape
    width = lat_w + STAT
    half, per = n // 2, n // SUBS
    messages = (half - 1) * SUBS + SUBS // 2
    any_spec = pl.BlockSpec(memory_space=pl.ANY)
    dma = pltpu.SemaphoreType.DMA
    out = pl.pallas_call(
        functools.partial(kernel, n, heads, lat_w, rope_w, page, slots),
        out_shape=pltpu.VMEM((heads, lat_w), bf16),
        in_specs=[any_spec] * 5 + [pl.BlockSpec(memory_space=pltpu.SMEM)],
        out_specs=pl.BlockSpec(memory_space=pltpu.VMEM),
        scratch_shapes=[
            pltpu.VMEM(cache_latent.shape, bf16),
            pltpu.VMEM(cache_rope.shape, bf16),
            pltpu.VMEM((2, n, n, heads, width), bf16),
            pltpu.VMEM((2, n, 8, 128), jnp.int32),
            pltpu.VMEM((n, n, heads, width), bf16),
            pltpu.VMEM((n, n, heads, width), bf16),
            pltpu.VMEM((n, n, heads, lat_w), f32),
            pltpu.VMEM((n, n, heads, STAT), f32),
            pltpu.VMEM((n, n, heads, STAT), f32),
            pltpu.VMEM((2, messages, per, heads, width), bf16),
            pltpu.VMEM((2, messages, per, heads, width), bf16),
            pltpu.VMEM((n, heads, width), bf16),
            pltpu.VMEM((n, heads, width), bf16),
            pltpu.VMEM((heads, width), bf16),
            pltpu.VMEM((8, 128), jnp.int32),
            pltpu.VMEM((heads, rope_w), bf16),
            pltpu.VMEM(page_table.shape, jnp.int32),
            pltpu.VMEM((8, 128), jnp.int32),
            pltpu.SMEM((8, 128), jnp.int32),
            dma((6,)),
            dma((n,)), dma((2, n)), dma((n,)), dma((2, n)),
            dma((2, 2, half * GSUBS)), dma((2, 2, half * GSUBS)),
            dma((2, 2, half * GSUBS)), dma((2, 2, half * GSUBS)),
            dma((3,)), dma((3,)),
            dma((n,)), dma((n,)),
            dma((2, messages)), dma((2, messages)),
            dma((n,)), dma((n,)),
        ],
        compiler_params=pltpu.CompilerParams(
            collective_id=0, has_side_effects=True, vmem_limit_bytes=57 * 1024 * 1024
        ),
    )(q_latent, q_rope, cache_latent, cache_rope, page_table, lengths)
    return out[None]


def solution(mesh):
    n = mesh.shape["head"]
    assert n == 8 and mesh.shape["seq"] == 2 * n
    placed = (
        P(("grp", "seq"), "head", None),
        P(("grp", "seq"), "head", None),
        P(("grp", "seq", "head"), None, None),
        P(("grp", "seq", "head"), None, None),
        P(("grp", "seq"), None),
        P(("grp", "seq")),
    )
    return jax.shard_map(
        functools.partial(on_device, n),
        mesh=mesh,
        in_specs=placed,
        out_specs=P(("grp", "seq"), "head", None),
        check_vma=False,
    )
```

```python
import functools

import jax
import jax.numpy as jnp
from jax import lax
from jax.experimental import pallas as pl
from jax.experimental.pallas import tpu as pltpu
from jax.sharding import PartitionSpec as P

softmax_scale = 0.13528
floor_score = -1e30
MESH = pl.DeviceIdType.MESH
MOST = 4
STAT = 128
SUBS = 4
GSUBS = 2
bf16, f32 = jnp.bfloat16, jnp.float32


def kernel(
    n, heads, lat_w, rope_w, page, slots,
    ql_hbm, qr_hbm, lat_hbm, rope_hbm, pt_hbm, len_ref,
    out_ref,
    lat, rope, QB, TB, SB, RB, LM, LT, LS, RR, MS, M2, FB, qown, town, qrv, ptv, tvm, tsm,
    loc, a_send, a_recv, t_send, t_recv, g_send, g_recv, d_send, d_recv, o_send, o_recv,
    p_send, p_recv, r_send, r_recv, f_send, f_recv,
):
    half = n // 2
    per = n // SUBS
    lanes = lat_w // 128
    sq = lax.axis_index("seq")
    x = lax.axis_index("head")
    y = sq // 2
    c = sq % 2
    a = x * (1 - c) + y * c
    b = y * (1 - c) + x * c

    def at(xx, yy, cc):
        return {"seq": 2 * yy + cc, "head": xx}

    def dev_a(i):
        return at(i * (1 - c) + x * c, y * (1 - c) + i * c, c)

    def dev_b(i):
        return at(x * (1 - c) + i * c, i * (1 - c) + y * c, c)

    sib = at(x, y, 1 - c)

    def rcopy(src, dst, ss, rs, dev):
        return pltpu.make_async_remote_copy(
            src_ref=src, dst_ref=dst, send_sem=ss, recv_sem=rs, device_id=dev, device_id_type=MESH
        )

    sends = []

    def send(src, dst, ss, rs, dev):
        cp = rcopy(src, dst, ss, rs, dev)
        cp.start()
        sends.append(cp)

    bar = pltpu.get_barrier_semaphore()
    far = sorted(range(1, n), key=lambda k: -min(k, n - k))
    partners = [at((x + k) % n, y, 1 - c) for k in far]
    partners += [at(x, (y + k) % n, 1 - c) for k in far]
    partners += [dev_a((a + k) % n) for k in far]
    partners += [dev_b((b + k) % n) for k in (1, 2, n - 2, n - 1)] + [sib]
    for dev in partners:
        pl.semaphore_signal(bar, inc=1, device_id=dev, device_id_type=MESH)

    cq = pltpu.make_async_copy(ql_hbm.at[0], qown.at[:, pl.ds(0, lat_w)], loc.at[0])
    cs = pltpu.make_async_copy(qr_hbm.at[0], qrv, loc.at[1])
    ct = pltpu.make_async_copy(pt_hbm, ptv, loc.at[2])
    cl = pltpu.make_async_copy(lat_hbm, lat, loc.at[3])
    cr = pltpu.make_async_copy(rope_hbm, rope, loc.at[4])
    ct.start()
    cs.start()
    cq.start()
    cl.start()
    cr.start()

    ct.wait()
    rows_t = []
    lane1 = lax.broadcasted_iota(jnp.int32, (1, 128), 1)
    entries = ptv.shape[1] // 128
    for r in range(entries):
        v = ptv[:, r * 128 : (r + 1) * 128]
        live = jnp.clip(len_ref[0] - (lane1 + r * 128) * page, 0, page)
        rows_t.append(jnp.where(v >= 0, v * 256 + live, -1))
    rows_t.append(jnp.full((8 - entries, 128), -1, jnp.int32))
    town[...] = jnp.concatenate(rows_t, axis=0)
    cs.wait()
    qown[:, pl.ds(lat_w, STAT)] = jnp.concatenate(
        [qrv[...], jnp.zeros((heads, STAT - rope_w), bf16)], axis=1
    )
    cq.wait()

    pl.semaphore_wait(bar, len(partners))

    for k in far:
        dev = at((x + k * (1 - c)) % n, (y + k * c) % n, 1)
        send(qown, QB.at[c, b, a], a_send.at[k], a_recv.at[c, k], dev)
    for k in far:
        send(town, TB.at[c, y], t_send.at[k], t_recv.at[c, k], at(x, (y + k) % n, 1))

    def part_of(par, idx, p):
        return QB.at[par, idx, pl.ds(p * (n // GSUBS), n // GSUBS)]

    order = (
        tuple(range(GSUBS)),
        tuple(range(GSUBS // 2, GSUBS)) + tuple(range(GSUBS // 2)),
    )
    mid = (y, x)

    def origin(par, d, k):
        return (mid[par] + n - k) % n if d == 0 else (mid[par] + k) % n

    def subs_at(k):
        return GSUBS // 2 if k == half else GSUBS

    def build_table():
        first = (sq * n + x) * slots * 256
        codes = TB[...].reshape(n * 16, 128)
        ok = (codes >= first) & (codes < first + slots * 256)
        key = jnp.where(ok, codes - first, -1).T
        keys = [key] + [pltpu.roll(key, 128 - r, 1) for r in range(1, entries)]
        row = lax.broadcasted_iota(jnp.int32, (8, 128), 0)
        res = jnp.full((8, 128), -1, jnp.int32)
        for j in range(MOST):
            m = functools.reduce(jnp.maximum, keys)
            size = m.shape[0]
            while size > 8:
                size //= 2
                m = jnp.maximum(m[:size], m[size:])
            for r in (4, 2, 1):
                m = jnp.maximum(m, pltpu.roll(m, r, 0))
            res = jnp.where(row == j, m, res)
            full = jnp.concatenate([m] * (n * 2), axis=0)
            keys = [jnp.where(v == full, -1, v) for v in keys]
        tvm[...] = res
        cp = pltpu.make_async_copy(tvm, tsm, loc.at[5])
        cp.start()
        return cp

    def stats(top, total):
        hi = total.astype(bf16)
        lo = (total - hi.astype(f32)).astype(bf16)
        lane = lax.broadcasted_iota(jnp.int32, top.shape, 1)
        st = jnp.where(lane == 0, top, jnp.where(lane == 1, hi.astype(f32), lo.astype(f32)))
        return st.astype(bf16)

    def attend(par, yy):
        q = (QB[0, yy] if par == 0 else QB[1, :, yy]).reshape(n * heads, -1)
        ql, qr = q[:, :lat_w], q[:, lat_w : lat_w + rope_w]
        pages, ropes, counts = [], [], []
        for j in range(MOST):
            code = tsm[j, 8 * (par * n + yy)]
            slot = jnp.maximum(code, 0) // 256
            counts.append(jnp.where(code < 0, 0, code % 256))
            pages.append(lat[slot])
            ropes.append(rope[slot])
        keys = jnp.concatenate(pages, axis=0)
        sc = lax.dot_general(ql, keys, (((1,), (1,)), ((), ())), preferred_element_type=f32)
        sc = sc + jnp.dot(qr, jnp.concatenate(ropes, axis=1), preferred_element_type=f32)
        lane = lax.broadcasted_iota(jnp.int32, (n * heads, page), 1)
        live = [lane < v for v in counts]
        parts = [
            jnp.where(live[j], sc[:, j * page : (j + 1) * page] * softmax_scale, floor_score)
            for j in range(MOST)
        ]
        top = functools.reduce(jnp.maximum, parts)
        top = jnp.max(top, axis=1, keepdims=True).astype(bf16).astype(f32)
        ws = [jnp.where(o, jnp.exp(s - top), 0.0) for o, s in zip(live, parts)]
        total = jnp.sum(ws[0] + ws[1] + ws[2] + ws[3], axis=1, keepdims=True)
        w = jnp.concatenate([v.astype(bf16) for v in ws], axis=1)
        mixed = jnp.dot(w, keys, preferred_element_type=f32)
        top = jnp.broadcast_to(top, (n * heads, STAT))
        total = jnp.broadcast_to(total, (n * heads, STAT))
        return mixed, top, total

    def keep(par, yy, own, state):
        mixed, top, total = state
        shape = (n, heads, -1)

        if own and par == 0:
            LM[yy] = mixed.reshape(shape)
            LT[yy] = top.reshape(shape)
            LS[yy] = total.reshape(shape)
        elif own:
            LM[:, yy] = mixed.reshape(shape)
            LT[:, yy] = top.reshape(shape)
            LS[:, yy] = total.reshape(shape)
        else:
            full = jnp.concatenate([mixed.astype(bf16), stats(top, total)], axis=1)
            SB[yy] = full.reshape(shape)

    def push(par, yy):
        dst = RB.at[yy] if par == 0 else RB.at[:, yy]
        rcopy(SB.at[yy], dst, p_send.at[yy], p_recv.at[yy], sib).start()

    def compute(par, own, *seqs):
        states = [attend(par, yy) for yy in seqs]
        for yy, state in zip(seqs, states):
            keep(par, yy, own, state)
        if not own:
            for yy in seqs:
                push(par, yy)

    rows = per * heads
    er = lax.broadcasted_iota(jnp.int32, (STAT, 2 * STAT), 0)
    ec = lax.broadcasted_iota(jnp.int32, (STAT, 2 * STAT), 1)
    spread = jnp.where(
        ((er == 0) & (ec < STAT)) | ((er > 0) & (er < 3) & (ec >= STAT)), 1.0, 0.0
    ).astype(bf16)

    def opened(v):
        s = jnp.dot(v[:, lat_w:], spread, preferred_element_type=f32)
        tiles = [v[:, j * 128 : (j + 1) * 128].astype(f32) for j in range(lanes)]
        return tiles, s[:, :STAT], s[:, STAT:]

    def merge(states):
        top = functools.reduce(jnp.maximum, [s[1] for s in states])
        fac = [jnp.exp(s[1] - top) for s in states]
        total = sum(f * s[2] for f, s in zip(fac, states))
        tiles = [sum(f * s[0][j] for f, s in zip(fac, states)) for j in range(lanes)]
        return tiles, top, total

    def packed(state):
        tiles, top, total = state
        return jnp.concatenate([t.astype(bf16) for t in tiles] + [stats(top, total)], axis=1)

    def ps(p):
        return pl.ds(p * per, per)

    def both(idx, p):
        v = LM[idx, ps(p)].reshape(rows, lat_w)
        tiles = [v[:, j * 128 : (j + 1) * 128] for j in range(lanes)]
        top = LT[idx, ps(p)].reshape(rows, STAT)
        total = LS[idx, ps(p)].reshape(rows, STAT)
        return [(tiles, top, total), opened(RB[idx, ps(p)].reshape(rows, -1))]

    def goal(d, k):
        return (b + k) % n if d == 0 else (b + n - k) % n

    halves = (
        (tuple(range(SUBS // 2, SUBS)), tuple(range(SUBS // 2))),
        (tuple(range(SUBS // 2)), tuple(range(SUBS // 2, SUBS))),
    )

    def reduce(need):
        out = []

        def put(src, dst, ss, rs, dev):
            cp = rcopy(src, dst, ss, rs, dev)
            cp.start()
            out.append(cp)

        def index(k, p):
            return {4: p % (SUBS // 2), 3: SUBS // 2, 2: SUBS // 2 + SUBS, 1: SUBS // 2 + 2 * SUBS}[
                k
            ] + (p if k < half else 0)

        def wait(d, k, p):
            i = index(k, p)
            part = RR.at[d, i]
            rcopy(part, part, r_send.at[d, i], r_recv.at[d, i], sib).wait_recv()

        def got(d, k, p):
            return [opened(RR[d, index(k, p)].reshape(rows, -1))]

        def step(k, subs, comes=()):
            states = [both(goal(d, k), subs[d]) for d in range(2)]
            for d in range(2):
                for g in comes:
                    wait(d, g, subs[d])
            for g in comes:
                states = [states[d] + got(d, g, subs[d]) for d in range(2)]
            full = [packed(merge(v)) for v in states]
            for d in range(2):
                MS[d, index(k, subs[d])] = full[d].reshape(per, heads, -1)
            for d in range(2):
                i, hops = index(k, subs[d]), 2 - k % 2
                dev = dev_b((b + (hops if d == 0 else n - hops)) % n)
                put(MS.at[d, i], RR.at[d, i], r_send.at[d, i], r_recv.at[d, i], dev)

        first, late = [tuple(zip(halves[0][h], halves[1][h])) for h in range(2)]
        for j in range(2):
            for i in need[j]:
                rcopy(RB.at[i], RB.at[i], p_send.at[i], p_recv.at[i], sib).wait_recv()
            step(4, late[j])
            step(3, first[j])
            step(3, late[j])
            step(1, first[j])
            step(1, late[j])
        for subs in first:
            step(2, subs, (3,))
        for subs in late:
            step(2, subs, (3, 4))
        for j in range(0, SUBS, 2):
            states = [both(b, p) for p in (j, j + 1)]
            for k in (1, 2):
                for p in (j, j + 1):
                    for d in range(2):
                        wait(d, k, p)
            full = [
                packed(merge(v + [g for k in (1, 2) for d in range(2) for g in got(d, k, p)]))
                for v, p in zip(states, (j, j + 1))
            ]
            for v, p in zip(full, (j, j + 1)):
                M2[ps(p)] = v.reshape(per, heads, -1)
            for o in range(j * per, (j + 2) * per):
                k = (o + n - a) % n

                @pl.when(o != a)
                def _(o=o, k=k):
                    rcopy(M2.at[o], FB.at[k], f_send.at[k], f_recv.at[k], dev_a(o)).start()

        for k in far:
            rcopy(FB.at[k], FB.at[k], f_send.at[k], f_recv.at[k], sib).wait_recv()
        tiles, top, total = merge([opened(M2[a])] + [opened(FB[k]) for k in far])
        out_ref[...] = jnp.concatenate([(t / total).astype(bf16) for t in tiles], axis=1)
        for i in range(n):
            rcopy(SB.at[i], SB.at[i], p_send.at[i], p_recv.at[i], sib).wait_send()
        for k in far:
            rcopy(FB.at[k], FB.at[k], f_send.at[k], f_recv.at[k], sib).wait_send()
        for cp in out:
            cp.wait_send()

    @pl.when(c == 1)
    def _():
        out = []

        def put(src, dst, ss, rs, dev):
            cp = rcopy(src, dst, ss, rs, dev)
            cp.start()
            out.append(cp)

        neighbour = (
            (at(x, (y + 1) % n, 1), at(x, (y + n - 1) % n, 1)),
            (at((x + 1) % n, y, 1), at((x + n - 1) % n, y, 1)),
        )
        QB[1, x, y] = qown[...]
        TB[1, y] = town[...]
        for par in (1, 0):
            for k in far + ([0] if par == 0 else []):
                src = (x + n - k) % n if par == 0 else (y + n - k) % n
                part = QB.at[par, mid[par], src]
                rcopy(part, part, a_send.at[k], a_recv.at[par, k], sib).wait_recv()
            for j in range(GSUBS):
                for d in range(2):
                    p = order[d][j]
                    part = part_of(par, mid[par], p)
                    put(part, part, g_send.at[par, d, p], g_recv.at[par, d, p], neighbour[par][d])
            part = QB.at[par, mid[par]]
            put(part, part, o_send.at[par], o_recv.at[par], sib)
        def ring_sub(k, j):
            for par in (1, 0):
                for d in range(2):
                    p = order[d][j]
                    i = (k - 1) * GSUBS + p
                    part = part_of(par, origin(par, d, k), p)
                    rcopy(part, part, g_send.at[par, d, i], g_recv.at[par, d, i], sib).wait_recv()
                    if k < half - 1 or (k == half - 1 and j < GSUBS // 2):
                        i2 = i + GSUBS
                        ss, rs = g_send.at[par, d, i2], g_recv.at[par, d, i2]
                        put(part, part, ss, rs, neighbour[par][d])
                    put(part, part, d_send.at[par, d, i], d_recv.at[par, d, i], sib)

        def ring_all(k):
            for j in range(subs_at(k)):
                ring_sub(k, j)

        for par in (1, 0):
            for k in far + ([0] if par == 0 else []):
                part = TB.at[par, (y + n - k) % n]
                rcopy(part, part, t_send.at[k], t_recv.at[par, k], sib).wait_recv()
        put(TB, TB, o_send.at[2], o_recv.at[2], sib)
        built = build_table()
        cl.wait()
        cr.wait()
        built.wait()
        compute(0, False, y)
        ring_all(1)
        compute(0, False, (y + 1) % n)
        ring_all(2)
        compute(0, False, (y + n - 1) % n)
        ring_all(3)
        compute(0, False, (y + 2) % n)
        ring_all(half)
        compute(0, False, (y + n - 2) % n, (y + half) % n)
        compute(0, False, (y + n - 3) % n, (y + 3) % n)

        def odd(i, carry):
            first = 4 * (i % 2) + 2 * (i // 2)
            compute(1, True, first, first + 1)
            return carry

        lax.fori_loop(0, n // 2, odd, 0)
        reduce(((0, 1, 4, 5), (2, 3, 6, 7)))
        for cp in out:
            cp.wait_send()

    @pl.when(c == 0)
    def _():
        put_a = rcopy(qown, QB.at[0, y, x], a_send.at[0], a_recv.at[0, 0], sib)
        put_t = rcopy(town, TB.at[0, y], t_send.at[0], t_recv.at[0, 0], sib)
        put_a.start()
        put_t.start()

        def arrived(par, k):
            if k == 0:
                part = QB.at[par, mid[par]]
                rcopy(part, part, o_send.at[par], o_recv.at[par], sib).wait_recv()
                return
            for j in range(subs_at(k)):
                for d in range(2):
                    p = order[d][j]
                    i = (k - 1) * GSUBS + p
                    part = part_of(par, origin(par, d, k), p)
                    rcopy(part, part, d_send.at[par, d, i], d_recv.at[par, d, i], sib).wait_recv()

        rcopy(TB, TB, o_send.at[2], o_recv.at[2], sib).wait_recv()
        built = build_table()
        cl.wait()
        cr.wait()
        arrived(0, 0)
        built.wait()
        compute(0, True, y)
        for k in range(1, half + 1):
            arrived(0, k)
            if k < half:
                compute(0, True, (y + n - k) % n, (y + k) % n)
            else:
                compute(0, True, (y + half) % n)
        for k in range(half + 1):
            arrived(1, k)

        def odd(i, carry):
            first = 4 * (i % 2) + 2 * (i // 2)
            compute(1, False, first, first + 1)
            return carry

        lax.fori_loop(0, n // 2, odd, 0)
        reduce((tuple(range(n)), ()))
        put_a.wait_send()
        put_t.wait_send()

    for cp in sends:
        cp.wait_send()


def on_device(n, q_latent, q_rope, cache_latent, cache_rope, page_table, lengths):
    heads, lat_w = q_latent.shape[1:]
    rope_w = q_rope.shape[2]
    slots, page, _ = cache_latent.shape
    width = lat_w + STAT
    half, per = n // 2, n // SUBS
    messages = (half - 1) * SUBS + SUBS // 2
    any_spec = pl.BlockSpec(memory_space=pl.ANY)
    dma = pltpu.SemaphoreType.DMA
    out = pl.pallas_call(
        functools.partial(kernel, n, heads, lat_w, rope_w, page, slots),
        out_shape=pltpu.VMEM((heads, lat_w), bf16),
        in_specs=[any_spec] * 5 + [pl.BlockSpec(memory_space=pltpu.SMEM)],
        out_specs=pl.BlockSpec(memory_space=pltpu.VMEM),
        scratch_shapes=[
            pltpu.VMEM(cache_latent.shape, bf16),
            pltpu.VMEM(cache_rope.shape, bf16),
            pltpu.VMEM((2, n, n, heads, width), bf16),
            pltpu.VMEM((2, n, 8, 128), jnp.int32),
            pltpu.VMEM((n, n, heads, width), bf16),
            pltpu.VMEM((n, n, heads, width), bf16),
            pltpu.VMEM((n, n, heads, lat_w), f32),
            pltpu.VMEM((n, n, heads, STAT), f32),
            pltpu.VMEM((n, n, heads, STAT), f32),
            pltpu.VMEM((2, messages, per, heads, width), bf16),
            pltpu.VMEM((2, messages, per, heads, width), bf16),
            pltpu.VMEM((n, heads, width), bf16),
            pltpu.VMEM((n, heads, width), bf16),
            pltpu.VMEM((heads, width), bf16),
            pltpu.VMEM((8, 128), jnp.int32),
            pltpu.VMEM((heads, rope_w), bf16),
            pltpu.VMEM(page_table.shape, jnp.int32),
            pltpu.VMEM((8, 128), jnp.int32),
            pltpu.SMEM((8, 128), jnp.int32),
            dma((6,)),
            dma((n,)), dma((2, n)), dma((n,)), dma((2, n)),
            dma((2, 2, half * GSUBS)), dma((2, 2, half * GSUBS)),
            dma((2, 2, half * GSUBS)), dma((2, 2, half * GSUBS)),
            dma((3,)), dma((3,)),
            dma((n,)), dma((n,)),
            dma((2, messages)), dma((2, messages)),
            dma((n,)), dma((n,)),
        ],
        compiler_params=pltpu.CompilerParams(
            collective_id=0, has_side_effects=True, vmem_limit_bytes=57 * 1024 * 1024
        ),
    )(q_latent, q_rope, cache_latent, cache_rope, page_table, lengths)
    return out[None]


def solution(mesh):
    n = mesh.shape["head"]
    assert n == 8 and mesh.shape["seq"] == 2 * n
    placed = (
        P(("grp", "seq"), "head", None),
        P(("grp", "seq"), "head", None),
        P(("grp", "seq", "head"), None, None),
        P(("grp", "seq", "head"), None, None),
        P(("grp", "seq"), None),
        P(("grp", "seq")),
    )
    return jax.shard_map(
        functools.partial(on_device, n),
        mesh=mesh,
        in_specs=placed,
        out_specs=P(("grp", "seq"), "head", None),
        check_vma=False,
    )
```
